256 devices in a mesh: dp: 32 (over x, z), expert: 8 (over y, core).
Axes of the slice: x: 4, y: 4, z: 8, core: 2. Of those that a mesh axis runs over, the one named last changes fastest.
Arguments:
- tokens: bfloat16 [1024, 2048], P('expert'), may hold values from -6 to 6
- cotangent: bfloat16 [1024, 2048], P('expert'), may hold values from -0.75 to 0.75
- router_logits: float32 [1024, 2], P('expert'), may hold values from -6 to 6
- routes: int32 [1024, 2], P('expert'), may hold values from 0 to 7, all different within a row; in each aligned block of 128 rows (0 to 127, 128 to 255, ...) at most 48 rows name the same one
- gate_weight: bfloat16 [8, 7168, 2048], P('expert', 'dp'), may hold values from -0.125 to 0.125
- up_weight: bfloat16 [8, 7168, 2048], P('expert', 'dp'), may hold values from -0.125 to 0.125
- down_weight: bfloat16 [8, 7168, 2048], P('expert', 'dp'), may hold values from -0.0625 to 0.0625
- dir_gate: bfloat16 [8, 7168, 2048], P('expert', 'dp'), may hold values from -0.125 to 0.125
- dir_up: bfloat16 [8, 7168, 2048], P('expert', 'dp'), may hold values from -0.125 to 0.125
- dir_down: bfloat16 [8, 7168, 2048], P('expert', 'dp'), may hold values from -0.0625 to 0.0625
Outputs:
- mixed: bfloat16 [1024, 2048], P('expert')
- hvp_gate: float32 [8, 7168, 2048], P('expert', 'dp')
- hvp_up: float32 [8, 7168, 2048], P('expert', 'dp')
- hvp_down: float32 [8, 7168, 2048], P('expert', 'dp')
The draws below stay inside these ranges and needn't reach their ends.
Inputs may be any that keep to these rules, and one draw needn't show every extreme that they name: `routes`: each row names 2 different experts; among the 128 rows of one index of the expert axis no expert is named more than 48 times, and in every draw some block names some expert exactly 48 times.
All inputs are finite; a program needn't handle non-finite values.
Results may differ from the reference program's by a relative error of at most 0.0074.
Values may be sent and summed in bfloat16 or wider, within the bound.
No kernel may reach another device: no remote copies, remote signals or barrier semaphores. Data moves between devices by JAX's collectives and lax.ppermute only.
A program may use at most 64 MiB of HBM per device.

```python
import math
import jax
import jax.numpy as jnp
import numpy as np
from jax import lax

D = 2048
FF = 7168
TOP = 2
TOK_DEV = 128
EXPERTS = 8
CAP = 48
TOKENS = 1024


def levels(own_key, extent, shards, least, largest):
    loudness, own = 1.0, jax.random.fold_in(own_key, 6)
    for position, blocks in shards:
        heights = jnp.exp(jax.random.uniform(jax.random.fold_in(own, position), (blocks,), jnp.float32, least / len(shards), largest / len(shards)))
        loudness = loudness * jnp.repeat(heights, extent[position] // blocks).reshape([-1 if axis == position else 1 for axis in range(len(extent))])
    return loudness


def assign_block(key, own, number, rows, amount, top, most, lean):
    order = jax.random.permutation(key, amount)
    crowded, usual = shares(amount, rows * top, most, lean, True), shares(amount, rows * top, most, lean, False)
    places = jnp.arange(amount)

    def named(lengths, rotation):
        used = int((lengths > 0).sum())
        fixed = max(1, used // 4)
        moved = fixed + (places - fixed + rotation * (used - fixed)) % max(1, amount - fixed)
        return jnp.zeros((amount,), jnp.int32).at[order[jnp.where(places < fixed, places, moved)]].set(jnp.asarray(lengths, jnp.int32))

    lengths = jnp.where(number % 4 == 0, named(crowded, number // 4), named(usual, number - number // 4 - 1))
    mixed = jax.random.permutation(jax.random.fold_in(own, 3), amount)
    source_of, sink = mixed[0:amount // 2 * 2:2], mixed[1:amount // 2 * 2:2]
    room = jnp.minimum(lengths[source_of] - 1, most - lengths[sink]) // 2
    room = jnp.where((source_of == order[0]) | (sink == order[0]) | (lengths[sink] == 0), 0, jnp.maximum(room, 0))
    moved = jax.random.randint(jax.random.fold_in(own, 4), (amount // 2,), 0, 1 << 20) % (room + 1)
    lengths = lengths.at[source_of].add(-moved).at[sink].add(moved)
    labels = jnp.searchsorted(jnp.cumsum(lengths), jnp.arange(rows * top), side="right").astype(jnp.int32)
    grid = labels.reshape(top, rows).T
    grid = grid[jax.random.permutation(jax.random.fold_in(own, 1), rows)]
    rotation = jax.random.randint(jax.random.fold_in(own, 2), (rows, 1), 0, top)
    return jnp.take_along_axis(grid, (jnp.arange(top)[None, :] + rotation) % top, axis=1)


def shares(count, total, reach, skew, full):
    portions = [(1 << 20) // math.isqrt(grade ** skew) + 1 for grade in range(1, count + 1)]
    largest = reach if full else min(reach, max(-(-total // count), total * portions[0] // sum(portions)))
    least = 1 if total - largest >= count - 1 else 0
    holding, spare = [largest] + [least] * (count - 1), total - largest - least * (count - 1)
    while spare > 0:
        candidates = [i for i in range(1, count) if holding[i] < largest] or [i for i in range(1, count) if holding[i] < reach]
        whole, left = sum([portions[i] for i in candidates]), spare
        for i in candidates:
            extra = min(reach - holding[i], max(1, left * portions[i] // whole), spare)
            holding[i] = holding[i] + extra
            spare = spare - extra
    return np.array(holding)


def gaussian(key, shape, width, most, shards=(), kind=jnp.bfloat16):
    array = width * jax.random.normal(key, shape, jnp.float32)
    if shards:
        array = array * levels(key, shape, shards, -0.22, 0.18)
    return jnp.clip(array, -most, most).astype(kind)


def setup_inputs(seed: int = 0) -> dict:
    seeds = jax.random.split(jax.random.key(seed), 11)
    tokens = gaussian(seeds[0], (TOKENS, D), 1.0, 6.0, ((0, 8),))
    cotangent = gaussian(seeds[1], (TOKENS, D), 0.125, 0.75, ((0, 8),))
    router_logits = gaussian(seeds[2], (TOKENS, TOP), 1.0, 6.0, ((0, 8),), jnp.float32)
    routes_keys = jax.random.split(jax.random.fold_in(seeds[3], 1), TOKENS // TOK_DEV)
    routes_turns = jax.random.permutation(jax.random.fold_in(seeds[3], 3), TOKENS // TOK_DEV)
    routes = jax.vmap(lambda own, number: assign_block(jax.random.fold_in(seeds[3], 2), own, number, TOK_DEV, EXPERTS, TOP, CAP, 2))(routes_keys, routes_turns).reshape((TOKENS, TOP))
    gate_weight = gaussian(seeds[4], (EXPERTS, FF, D), D ** -0.5, 0.125, ((0, 8), (1, 32)))
    up_weight = gaussian(seeds[5], (EXPERTS, FF, D), D ** -0.5, 0.125, ((0, 8), (1, 32)))
    down_weight = gaussian(seeds[6], (EXPERTS, FF, D), FF ** -0.5, 0.0625, ((0, 8), (1, 32)))
    dir_gate = gaussian(seeds[7], (EXPERTS, FF, D), D ** -0.5, 0.125, ((0, 8), (1, 32)))
    dir_up = gaussian(seeds[8], (EXPERTS, FF, D), D ** -0.5, 0.125, ((0, 8), (1, 32)))
    dir_down = gaussian(seeds[9], (EXPERTS, FF, D), FF ** -0.5, 0.0625, ((0, 8), (1, 32)))
    return dict(tokens=tokens, cotangent=cotangent, router_logits=router_logits, routes=routes, gate_weight=gate_weight, up_weight=up_weight, down_weight=down_weight, dir_gate=dir_gate, dir_up=dir_up, dir_down=dir_down)


def derivatives(preact):
    sigmoid_value = jax.nn.sigmoid(preact)
    slope_one = sigmoid_value * (1.0 + preact * (1.0 - sigmoid_value))
    slope_two = sigmoid_value * (1.0 - sigmoid_value) * (2.0 + preact * (1.0 - 2.0 * sigmoid_value))
    return preact * sigmoid_value, slope_one, slope_two


def project(left_rows, matrix):
    return jnp.einsum("rd,hd->rh", left_rows, matrix, preferred_element_type=jnp.float32)


def outer_sum(left_rows, right_rows):
    return jnp.einsum("rh,rd->hd", left_rows, right_rows, preferred_element_type=jnp.float32)


def block_terms(weights, token_rows, cot_rows):
    gate_mat, up_mat, down_mat, gate_dir, up_dir, down_dir = weights
    preact = project(token_rows, gate_mat)
    up_value = project(token_rows, up_mat)
    back_grad = project(cot_rows, down_mat)
    tang_gate = project(token_rows, gate_dir)
    tang_up = project(token_rows, up_dir)
    back_tang = project(cot_rows, down_dir)
    silu_value, slope_one, slope_two = derivatives(preact)
    hidden = (silu_value * up_value).astype(jnp.bfloat16)
    silu_tang = slope_one * tang_gate
    hidden_tang = (silu_tang * up_value + silu_value * tang_up).astype(jnp.bfloat16)
    resid_gate = ((back_tang * up_value + back_grad * tang_up) * slope_one + back_grad * up_value * slope_two * tang_gate).astype(jnp.bfloat16)
    resid_up = (back_tang * silu_value + back_grad * silu_tang).astype(jnp.bfloat16)
    return hidden, outer_sum(resid_gate, token_rows), outer_sum(resid_up, token_rows), outer_sum(hidden_tang, cot_rows)


def reference(tokens, cotangent, router_logits, routes, gate_weight, up_weight, down_weight, dir_gate, dir_up, dir_down):
    sources = TOKENS // TOK_DEV
    gate_first = jax.nn.sigmoid(router_logits[:, 0] - router_logits[:, 1])
    gate_prob = jnp.stack([gate_first, 1.0 - gate_first], axis=1)
    onehot = (routes.reshape(sources, TOK_DEV * TOP)[:, :, None] == jnp.arange(EXPERTS, dtype=jnp.int32)[None, None, :]).astype(jnp.int32)
    earlier = jnp.cumsum(onehot, axis=1) - onehot
    slot_pos = jnp.sum(earlier * onehot, axis=2).reshape(TOKENS, TOP)
    source = (jnp.arange(TOKENS, dtype=jnp.int32) // TOK_DEV)[:, None]
    slot_index = ((routes * sources + source) * CAP + slot_pos).reshape(-1).astype(jnp.int32)
    scaled = (gate_prob[:, :, None] * cotangent.astype(jnp.float32)[:, None, :]).astype(jnp.bfloat16).reshape(TOKENS * TOP, D)
    repeated = jnp.repeat(tokens, TOP, axis=0)
    total_slots = EXPERTS * sources * CAP
    slot_x = jnp.zeros((total_slots, D), jnp.bfloat16).at[slot_index].set(repeated).reshape(EXPERTS, sources * CAP, D)
    slot_c = jnp.zeros((total_slots, D), jnp.bfloat16).at[slot_index].set(scaled).reshape(EXPERTS, sources * CAP, D)

    def expert_pass(operands):
        token_rows, cot_rows = operands[0], operands[1]
        weights = operands[2:]
        hidden, part_gate, part_up, part_down = block_terms(weights, token_rows, cot_rows)
        expert_out = jnp.dot(hidden, weights[2], preferred_element_type=jnp.float32).astype(jnp.bfloat16)
        return expert_out, part_gate, part_up, part_down

    expert_out, hvp_gate, hvp_up, hvp_down = lax.map(expert_pass, (slot_x, slot_c, gate_weight, up_weight, down_weight, dir_gate, dir_up, dir_down))
    picked = expert_out.reshape(total_slots, D)[slot_index].astype(jnp.float32).reshape(TOKENS, TOP, D)
    mixed = jnp.sum(gate_prob[:, :, None] * picked, axis=1).astype(jnp.bfloat16)
    return (mixed, hvp_gate, hvp_up, hvp_down)
```

```python
import jax
import jax.numpy as jnp
from jax import lax
from jax.experimental import pallas as pl
from jax.experimental.pallas import tpu as pltpu
from jax.sharding import Mesh, PartitionSpec as P

F32, BF16, I32 = jnp.float32, jnp.bfloat16, jnp.int32
CAP = 48
EXPERTS = 8
SPLIT = 8
FAR = 4
VMEM_LIMIT = 40 * 1024 * 1024

NEAR_AXES = ("x", "zl")
BACK_AXES = ("zh", "y", "c")
DP_AXES = ("x", "zh", "zl")
EXPERT_AXES = ("y", "c")


def call(body, outs, name):
    return pl.pallas_call(
        body,
        out_shape=outs,
        name=name,
        compiler_params=pltpu.CompilerParams(vmem_limit_bytes=VMEM_LIMIT),
    )


def iota(shape, dim):
    return lax.broadcasted_iota(I32, shape, dim)


def slots_of(routes):
    first, second = routes[0:1, :], routes[1:2, :]
    tok = routes.shape[1]
    experts = iota((EXPERTS, tok), 0)
    is_first, is_second = experts == first, experts == second
    member = jnp.where(is_first | is_second, 1.0, 0.0).astype(BF16)
    before = jnp.where(iota((tok, tok), 0) < iota((tok, tok), 1), 1.0, 0.0).astype(BF16)
    count = jnp.dot(member, before, preferred_element_type=F32)
    pos_first = jnp.sum(jnp.where(is_first, count, 0.0), axis=0, keepdims=True).astype(I32)
    pos_second = jnp.sum(jnp.where(is_second, count, 0.0), axis=0, keepdims=True).astype(I32)
    return first, second, pos_first, pos_second


def gate_probs(logits):
    first = jax.nn.sigmoid(logits[0:1, :] - logits[1:2, :])
    return first, 1.0 - first


def send_tokens_body(routes_ref, tok_ref, out_ref):
    first, second, pos_first, pos_second = slots_of(routes_ref[...])
    tok = tok_ref.shape[0]
    rows = iota((EXPERTS * CAP, tok), 0)
    hit = (rows == first * CAP + pos_first) | (rows == second * CAP + pos_second)
    dispatch = jnp.where(hit, 1.0, 0.0).astype(BF16)
    out = jnp.dot(dispatch, tok_ref[...], preferred_element_type=F32)
    out_ref[...] = out.astype(BF16).reshape(out_ref.shape)


def send_cot_body(me_ref, routes_ref, logits_ref, cot_ref, *out_refs):
    me = me_ref[0]
    first, second, pos_first, pos_second = slots_of(routes_ref[...])
    prob_first, prob_second = gate_probs(logits_ref[...])
    tok = cot_ref.shape[0]
    rows = iota((EXPERTS * CAP, tok), 0)
    hit_first = rows == (first ^ me) * CAP + pos_first
    hit_second = rows == (second ^ me) * CAP + pos_second
    dispatch = jnp.where(hit_first | hit_second, 1.0, 0.0).astype(BF16)
    weight = jnp.where(hit_first, prob_first, 0.0) + jnp.where(hit_second, prob_second, 0.0)
    weight = jnp.sum(weight, axis=1, keepdims=True)
    picked = jnp.dot(dispatch, cot_ref[...], preferred_element_type=F32)
    scaled = (picked * weight).astype(BF16)
    for i, out_ref in enumerate(out_refs):
        out_ref[...] = scaled[i * CAP : (i + 1) * CAP]


def place_body(me_ref, *refs):
    out_ref = refs[-1]
    me = me_ref[0]
    for i, ref in enumerate(refs[:-1]):
        out_ref[me ^ i] = ref[...]


def nt_dot(rows, matrix):
    return lax.dot_general(rows, matrix, (((1,), (1,)), ((), ())), preferred_element_type=F32)


def forward_body(x_ref, gate_ref, up_ref, down_ref, pre_ref, up_out_ref, part_ref):
    rows = x_ref[...]
    pre = nt_dot(rows, gate_ref[...])
    up_value = nt_dot(rows, up_ref[...])
    pre_ref[...] = pre
    up_out_ref[...] = up_value
    hidden = (pre * jax.nn.sigmoid(pre) * up_value).astype(BF16)
    width = part_ref.shape[2]
    for j in range(SPLIT):
        part = jnp.dot(
            hidden, down_ref[:, j * width : (j + 1) * width], preferred_element_type=F32
        )
        part_ref[j] = part.astype(BF16)


def near_sum_body(part_ref, out_ref):
    half = CAP // 2
    total = part_ref[0].astype(F32)
    for j in range(1, SPLIT):
        total = total + part_ref[j].astype(F32)
    left = iota((half, 128), 1) < 64
    for s in range(EXPERTS):
        for m in range(2):
            cols = slice(128 * m, 128 * m + 128)
            upper = total[s * CAP : s * CAP + half, cols]
            lower = total[s * CAP + half : (s + 1) * CAP, cols]
            even = jnp.where(left, upper, pltpu.roll(lower, 64, 1))
            odd = jnp.where(left, pltpu.roll(upper, 64, 1), lower)
            out_ref[2 * m * EXPERTS + s] = even.astype(BF16)
            out_ref[(2 * m + 1) * EXPERTS + s] = odd.astype(BF16)


def combine_body(routes_ref, logits_ref, back_ref, out_ref):
    half = CAP // 2
    first, second, pos_first, pos_second = slots_of(routes_ref[...])
    prob_first, prob_second = gate_probs(logits_ref[...])
    tok = routes_ref.shape[1]
    total = back_ref[0:EXPERTS].astype(F32)
    for z in range(1, FAR):
        total = total + back_ref[z * EXPERTS : (z + 1) * EXPERTS].astype(F32)
    held = total.astype(BF16).reshape(EXPERTS * half, 128)
    rows = iota((EXPERTS * half, tok), 0)

    def pick(expert, pos):
        base = expert * half + pos
        in_upper = jnp.where((rows == base) & (pos < half), 1.0, 0.0).astype(BF16)
        in_lower = jnp.where((rows == base - half) & (pos >= half), 1.0, 0.0).astype(BF16)
        dims = (((0,), (0,)), ((), ()))
        from_upper = lax.dot_general(held, in_upper, dims, preferred_element_type=F32)
        from_lower = lax.dot_general(held, in_lower, dims, preferred_element_type=F32)
        return from_upper[0:64] + from_lower[64:128]

    mixed = prob_first * pick(first, pos_first) + prob_second * pick(second, pos_second)
    mixed = mixed.astype(BF16)
    for j in range(out_ref.shape[0]):
        out_ref[j] = mixed


def turn_body(in_ref, out_ref):
    for m in range(out_ref.shape[1] // 128):
        block = in_ref[2 * m : 2 * m + 2].reshape(128, 128)
        out_ref[:, 128 * m : 128 * m + 128] = block.T


def derivatives(preact):
    sigmoid_value = jax.nn.sigmoid(preact)
    slope_one = sigmoid_value * (1.0 + preact * (1.0 - sigmoid_value))
    slope_two = sigmoid_value * (1.0 - sigmoid_value) * (2.0 + preact * (1.0 - 2.0 * sigmoid_value))
    return (preact * sigmoid_value, slope_one, slope_two)


def outer_sum(left_rows, right_rows):
    return jnp.einsum("rh,rd->hd", left_rows, right_rows, preferred_element_type=F32)


def shards(
    tokens,
    cotangent,
    router_logits,
    routes,
    gate_weight,
    up_weight,
    down_weight,
    dir_gate,
    dir_up,
    dir_down,
):
    tok, width = tokens.shape
    rows = EXPERTS * CAP
    units = gate_weight.shape[1]
    sds = jax.ShapeDtypeStruct
    routes_t = routes.T
    logits_t = router_logits.T
    me = (lax.axis_index("y") * 2 + lax.axis_index("c")).astype(I32).reshape(1)
    gate_mat, up_mat, down_mat = gate_weight[0], up_weight[0], down_weight[0]
    gate_dir, up_dir, down_dir = dir_gate[0], dir_up[0], dir_down[0]

    send_x = call(send_tokens_body, sds((EXPERTS, CAP, width), BF16), "send_tokens")(
        routes_t, tokens
    )
    slot_x = lax.all_to_all(send_x, EXPERT_AXES, 0, 0, tiled=True).reshape(rows, width)

    smem = pl.BlockSpec(memory_space=pltpu.SMEM)
    vmem = pl.BlockSpec(memory_space=pltpu.VMEM)
    params = pltpu.CompilerParams(vmem_limit_bytes=VMEM_LIMIT)
    send_c = pl.pallas_call(
        send_cot_body,
        out_shape=[sds((CAP, width), BF16)] * EXPERTS,
        in_specs=[smem, vmem, vmem, vmem],
        compiler_params=params,
        name="send_cot",
    )(me, routes_t, logits_t, cotangent)

    preact, up_value, partial_out = call(
        forward_body,
        [
            sds((rows, units), F32),
            sds((rows, units), F32),
            sds((SPLIT, rows, width // SPLIT), BF16),
        ],
        "forward",
    )(slot_x, gate_mat, up_mat, down_mat)

    near = lax.all_to_all(partial_out, NEAR_AXES, 0, 0, tiled=True)

    send_c, _ = lax.optimization_barrier((send_c, partial_out))
    pieces = [send_c[0]]
    for i in range(1, EXPERTS):
        pairs = [(d, d ^ i) for d in range(EXPERTS)]
        pieces.append(lax.ppermute(send_c[i], EXPERT_AXES, pairs))

    tang_gate = jnp.einsum("rd,hd->rh", slot_x, gate_dir, preferred_element_type=F32)
    tang_up = jnp.einsum("rd,hd->rh", slot_x, up_dir, preferred_element_type=F32)

    near_total = call(near_sum_body, sds((FAR * EXPERTS, CAP // 2, 128), BF16), "near_sum")(near)
    back = lax.all_to_all(near_total, BACK_AXES, 0, 0, tiled=True)

    slot_c = pl.pallas_call(
        place_body,
        out_shape=sds((EXPERTS, CAP, width), BF16),
        in_specs=[smem] + [vmem] * EXPERTS,
        compiler_params=params,
        name="place",
    )(me, *pieces).reshape(rows, width)

    back_grad = jnp.einsum("rd,hd->rh", slot_c, down_mat, preferred_element_type=F32)
    back_tang = jnp.einsum("rd,hd->rh", slot_c, down_dir, preferred_element_type=F32)
    silu_value, slope_one, slope_two = derivatives(preact)
    silu_tang = slope_one * tang_gate
    hidden_tang = (silu_tang * up_value + silu_value * tang_up).astype(BF16)
    resid_gate = (
        (back_tang * up_value + back_grad * tang_up) * slope_one
        + back_grad * up_value * slope_two * tang_gate
    ).astype(BF16)
    resid_up = (back_tang * silu_value + back_grad * silu_tang).astype(BF16)
    hvp_gate = outer_sum(resid_gate, slot_x)
    hvp_up = outer_sum(resid_up, slot_x)
    hvp_down = outer_sum(hidden_tang, slot_c)

    share = call(combine_body, sds((32, 64, tok), BF16), "combine")(routes_t, logits_t, back)
    full = lax.all_to_all(share, ("x", "zl", "zh"), 0, 0, tiled=True)
    mixed = call(turn_body, sds((tok, width), BF16), "turn")(full)
    return (mixed, hvp_gate[None], hvp_up[None], hvp_down[None])


def solution(mesh):
    grid = Mesh(mesh.devices.reshape(4, 4, 2, 4, 2), ("x", "zh", "zl", "y", "c"))
    by_expert = P(EXPERT_AXES, None)
    by_both = P(EXPERT_AXES, DP_AXES, None)
    return jax.shard_map(
        shards,
        mesh=grid,
        in_specs=(by_expert,) * 4 + (by_both,) * 6,
        out_specs=(by_expert,) + (by_both,) * 3,
        check_vma=False,
    )
```

```python
import jax
import jax.numpy as jnp
from jax import lax
from jax.experimental import pallas as pl
from jax.experimental.pallas import tpu as pltpu
from jax.sharding import Mesh, PartitionSpec as P

F32, BF16, I32 = jnp.float32, jnp.bfloat16, jnp.int32
CAP = 48
HALF = CAP // 2
EXPERTS = 8
X, Z, Y = 4, 8, 4
VMEM_LIMIT = 16 * 1024 * 1024

DP_AXES = ("x", "z")
EXPERT_AXES = ("y", "c")
BACK_AXES = ("z", "y", "c")

sds = jax.ShapeDtypeStruct
SMEM = pl.BlockSpec(memory_space=pltpu.SMEM)
VMEM = pl.BlockSpec(memory_space=pltpu.VMEM)
HBM = pl.BlockSpec(memory_space=pltpu.HBM)
ANY = pl.BlockSpec(memory_space=pl.ANY)


def call(body, ins, outs, scratch=(), mflops=0, **kwargs):
    specs, shapes = [pair[0] for pair in outs], [pair[1] for pair in outs]
    single = len(outs) == 1
    return pl.pallas_call(
        body,
        out_shape=shapes[0] if single else shapes,
        in_specs=ins,
        out_specs=specs[0] if single else specs,
        scratch_shapes=list(scratch),
        cost_estimate=pl.CostEstimate(
            flops=mflops * 1000000, bytes_accessed=4000000, transcendentals=0
        ),
        compiler_params=pltpu.CompilerParams(vmem_limit_bytes=VMEM_LIMIT),
        **kwargs,
    )


def in_hbm(value):
    return pltpu.with_memory_space_constraint(value, pltpu.HBM)


def dma(source, target, sem):
    copy = pltpu.make_async_copy(source, target, sem)
    copy.start()
    return copy


def iota(shape, dim):
    return lax.broadcasted_iota(I32, shape, dim)


def slots_of(routes):
    first, second = routes[0:1, :], routes[1:2, :]
    tok = routes.shape[1]
    experts = iota((EXPERTS, tok), 0)
    is_first, is_second = experts == first, experts == second
    member = jnp.where(is_first | is_second, 1.0, 0.0).astype(BF16)
    before = jnp.where(iota((tok, tok), 0) < iota((tok, tok), 1), 1.0, 0.0).astype(BF16)
    count = jnp.dot(member, before, preferred_element_type=F32)
    pos_first = jnp.sum(jnp.where(is_first, count, 0.0), axis=0, keepdims=True).astype(I32)
    pos_second = jnp.sum(jnp.where(is_second, count, 0.0), axis=0, keepdims=True).astype(I32)
    return first, second, pos_first, pos_second


def gate_probs(logits):
    first = jax.nn.sigmoid(logits[0:1, :] - logits[1:2, :])
    return first, 1.0 - first


def nt_dot(rows, matrix):
    return lax.dot_general(rows, matrix, (((1,), (1,)), ((), ())), preferred_element_type=F32)


def tn_dot(rows, matrix):
    return lax.dot_general(rows, matrix, (((0,), (0,)), ((), ())), preferred_element_type=F32)


def send_tokens_body(routes_hbm, tok_hbm, out_hbm, routes_ref, tok_ref, out_ref, sems):
    get_routes = dma(routes_hbm, routes_ref, sems.at[0])
    get_tok = dma(tok_hbm, tok_ref, sems.at[1])
    get_routes.wait()
    first, second, pos_first, pos_second = slots_of(routes_ref[...])
    tok = tok_ref.shape[0]
    rows = iota((EXPERTS * CAP, tok), 0)
    hit = (rows == first * CAP + pos_first) | (rows == second * CAP + pos_second)
    dispatch = jnp.where(hit, 1.0, 0.0).astype(BF16)
    get_tok.wait()
    tokens = tok_ref[...]
    puts = []
    part = EXPERTS // 2
    for j in range(2):
        picked = jnp.dot(
            dispatch[j * part * CAP : (j + 1) * part * CAP], tokens, preferred_element_type=F32
        )
        out_ref[j * part : (j + 1) * part] = picked.astype(BF16).reshape(part, CAP, -1)
        where = pl.ds(j * part, part)
        puts.append(dma(out_ref.at[where], out_hbm.at[where], sems.at[2 + j]))
    for put in puts:
        put.wait()


def send_cot_body(at_ref, *refs):
    routes_refs, logits_refs, cot_refs = refs[0:2], refs[2:4], refs[4:6]
    out_refs = refs[6:]
    y, c = at_ref[0], at_ref[1]
    for j in range(2):
        first, second, pos_first, pos_second = slots_of(routes_refs[j][...])
        prob_first, prob_second = gate_probs(logits_refs[j][...])
        tok = cot_refs[j].shape[0]
        rows = iota((Y * CAP, tok), 0)

        def hit(expert, pos):
            row = ((expert >> 1) ^ y) * CAP + pos
            return rows == jnp.where((expert & 1) == c, row, -1)

        hit_first, hit_second = hit(first, pos_first), hit(second, pos_second)
        dispatch = jnp.where(hit_first | hit_second, 1.0, 0.0).astype(BF16)
        weight = jnp.where(hit_first, prob_first, 0.0) + jnp.where(hit_second, prob_second, 0.0)
        weight = jnp.sum(weight, axis=1, keepdims=True)
        picked = jnp.dot(dispatch, cot_refs[j][...], preferred_element_type=F32)
        scaled = (picked * weight).astype(BF16)
        for i, out_ref in enumerate(out_refs):
            out_ref[j] = scaled[i * CAP : (i + 1) * CAP]


def split_down_body(at_ref, down_ref, *out_refs):
    me = at_ref[2]
    width = out_refs[0].shape[1]
    for i, out_ref in enumerate(out_refs):
        start = pl.multiple_of((me ^ i) * width, 128)
        out_ref[...] = down_ref[:, pl.ds(start, width)]


def forward_body(x_ref, gate_hbm, up_hbm, *refs):
    pre_hbm, value_hbm, hidden_ref, gate_ref, up_ref, pre_ref, value_ref, sems = refs[-8:]
    get_gate = dma(gate_hbm, gate_ref, sems.at[0])
    get_up = dma(up_hbm, up_ref, sems.at[1])
    rows = x_ref[...]
    get_gate.wait()
    pre = nt_dot(gate_ref[...], rows)
    pre_ref[...] = pre
    put_pre = dma(pre_ref, pre_hbm, sems.at[2])
    get_up.wait()
    value = nt_dot(up_ref[...], rows)
    value_ref[...] = value
    put_value = dma(value_ref, value_hbm, sems.at[3])
    hidden_ref[...] = (pre * jax.nn.sigmoid(pre) * value).astype(BF16)
    put_pre.wait()
    put_value.wait()


def down_body(*refs):
    hidden_refs, down_hbms, out_hbm = refs[:X], refs[X : 2 * X], refs[2 * X]
    down_refs, (out_ref, sems) = refs[2 * X + 1 : 3 * X + 1], refs[3 * X + 1 :]
    gets = [dma(a, b, sems.at[i]) for i, (a, b) in enumerate(zip(down_hbms, down_refs))]
    total = None
    for i in range(X):
        gets[i].wait()
        part = tn_dot(hidden_refs[i][...], down_refs[i][...])
        total = part if total is None else total + part
    left = iota((HALF, 128), 1) < 64
    puts = []
    for m in range(Z // 2):
        cols = slice(128 * m, 128 * m + 128)
        for s in range(EXPERTS):
            upper = total[s * CAP : s * CAP + HALF, cols]
            lower = total[s * CAP + HALF : (s + 1) * CAP, cols]
            even = jnp.where(left, upper, pltpu.roll(lower, 64, 1))
            odd = jnp.where(left, pltpu.roll(upper, 64, 1), lower)
            out_ref[2 * m * EXPERTS + s] = even.astype(BF16)
            out_ref[(2 * m + 1) * EXPERTS + s] = odd.astype(BF16)
        where = pl.ds(2 * m * EXPERTS, 2 * EXPERTS)
        puts.append(dma(out_ref.at[where], out_hbm.at[where], sems.at[X + m]))
    for put in puts:
        put.wait()


def combine_body(routes_ref, logits_ref, back_ref, _, out_ref):
    first, second, pos_first, pos_second = slots_of(routes_ref[...])
    prob_first, prob_second = gate_probs(logits_ref[...])
    tok = routes_ref.shape[1]
    total = back_ref[0:EXPERTS].astype(F32)
    for z in range(1, Z):
        total = total + back_ref[z * EXPERTS : (z + 1) * EXPERTS].astype(F32)
    held = total.astype(BF16).reshape(EXPERTS * HALF, 128)
    rows = iota((EXPERTS * HALF, tok), 0)

    def pick(expert, pos):
        base = expert * HALF + pos
        in_upper = jnp.where((rows == base) & (pos < HALF), 1.0, 0.0).astype(BF16)
        in_lower = jnp.where((rows == base - HALF) & (pos >= HALF), 1.0, 0.0).astype(BF16)
        return tn_dot(held, in_upper)[0:64] + tn_dot(held, in_lower)[64:128]

    mixed = prob_first * pick(first, pos_first) + prob_second * pick(second, pos_second)
    mixed = mixed.astype(BF16)
    for z in range(Z):
        out_ref[z] = mixed


def turn_body(at_ref, *refs):
    out_ref = refs[-1]
    me = at_ref[2]
    for i, ref in enumerate(refs[:-1]):
        rows = ref.shape[0] * ref.shape[1]
        block = ref[...].reshape(rows, ref.shape[2])
        for m in range(rows // 128):
            start = pl.multiple_of((me ^ i) * rows + 128 * m, 128)
            out_ref[:, pl.ds(start, 128)] = block[128 * m : 128 * m + 128].T


def tangent_body(
    x_ref, pre_ref, value_ref, gate_dir_ref, up_dir_ref, *out_refs
):
    by_tq_gate_ref, by_q_gate_ref, by_tq_up_ref, by_q_up_ref, hidden_tang_ref = out_refs
    rows = x_ref[...]
    tang_gate = nt_dot(gate_dir_ref[...], rows)
    tang_up = nt_dot(up_dir_ref[...], rows)
    pre, value = pre_ref[...], value_ref[...]
    sig = jax.nn.sigmoid(pre)
    slope_one = sig * (1.0 + pre * (1.0 - sig))
    slope_two = sig * (1.0 - sig) * (2.0 + pre * (1.0 - 2.0 * sig))
    silu = pre * sig
    silu_tang = slope_one * tang_gate
    by_tq_gate_ref[...] = value * slope_one
    by_q_gate_ref[...] = tang_up * slope_one + value * slope_two * tang_gate
    by_tq_up_ref[...] = silu
    by_q_up_ref[...] = silu_tang
    hidden_tang_ref[...] = (silu_tang * value + silu * tang_up).astype(BF16)


def residual_body(at_ref, down_ref, down_dir_ref, *refs):
    pieces, factors = refs[0:Y], refs[Y : Y + 4]
    slot_c_ref, resid_gate_ref, resid_up_ref = refs[Y + 4 :]
    by_tq_gate_ref, by_q_gate_ref, by_tq_up_ref, by_q_up_ref = factors
    y, c = at_ref[0], at_ref[1]
    for i, piece in enumerate(pieces):
        for j in range(2):
            start = pl.multiple_of((2 * (y ^ i) + (c ^ j)) * CAP, CAP)
            slot_c_ref[pl.ds(start, CAP), :] = piece[j]
    rows = slot_c_ref[...]
    back_grad = nt_dot(down_ref[...], rows)
    back_tang = nt_dot(down_dir_ref[...], rows)
    resid_gate = back_tang * by_tq_gate_ref[...] + back_grad * by_q_gate_ref[...]
    resid_up = back_tang * by_tq_up_ref[...] + back_grad * by_q_up_ref[...]
    resid_gate_ref[...] = resid_gate.astype(BF16)
    resid_up_ref[...] = resid_up.astype(BF16)


def outer_body(gate_units_ref, up_units_ref, down_units_ref, x_ref, c_ref, *refs):
    outs, holds, sems = refs[0:3], refs[3:6], refs[6]
    width = x_ref.shape[1]
    step = width // 4
    puts = []
    for g in range(4):
        cols = pl.ds(g * step, step)
        for k, (units_ref, rows_ref) in enumerate(
            ((gate_units_ref, x_ref), (up_units_ref, x_ref), (down_units_ref, c_ref))
        ):
            holds[k][0, :, cols] = jnp.dot(
                units_ref[...], rows_ref[:, cols], preferred_element_type=F32
            )
            puts.append(
                dma(holds[k].at[:, :, cols], outs[k].at[:, :, cols], sems.at[3 * g + k])
            )
    for put in puts:
        put.wait()


def spread(pieces, axes):
    arrived = [pieces[0]]
    for i in range(1, len(pieces)):
        pairs = [(d, d ^ i) for d in range(len(pieces))]
        arrived.append(lax.ppermute(pieces[i], axes, pairs))
    return arrived


def exchange(value, axes):
    return lax.all_to_all(value, axes, 0, 0, tiled=True)


def shards(
    tokens,
    cotangent,
    router_logits,
    routes,
    gate_weight,
    up_weight,
    down_weight,
    dir_gate,
    dir_up,
    dir_down,
):
    tok, width = tokens.shape
    rows = EXPERTS * CAP
    units = gate_weight.shape[1]
    quarter = width // X
    routes_t, logits_t = routes.T, router_logits.T
    at = jnp.stack([lax.axis_index("y"), lax.axis_index("c"), lax.axis_index("x")]).astype(I32)
    down_mat = down_weight[0]
    gate_dir, up_dir, down_dir = dir_gate[0], dir_up[0], dir_down[0]
    dma_sems = pltpu.SemaphoreType.DMA

    send_x = call(
        send_tokens_body,
        [HBM, HBM],
        [(HBM, pltpu.HBM((EXPERTS, CAP, width), BF16))],
        [
            pltpu.VMEM((2, tok), I32),
            pltpu.VMEM((tok, width), BF16),
            pltpu.VMEM((EXPERTS, CAP, width), BF16),
            dma_sems((4,)),
        ],
        mflops=200,
    )(in_hbm(routes_t), in_hbm(tokens))
    slot_x = exchange(send_x, EXPERT_AXES).reshape(rows, width)

    send_down = call(
        split_down_body, [SMEM, VMEM], [(VMEM, pltpu.HBM((units, quarter), BF16))] * X, mflops=200
    )(at, in_hbm(down_mat))
    down_parts = spread(send_down, "x")
    routes_two, logits_two, cot_two = (
        spread([value] * 2, "c") for value in (routes_t, logits_t, cotangent)
    )
    send_c = call(
        send_cot_body,
        [SMEM] + [VMEM] * 6,
        [(VMEM, pltpu.HBM((2, CAP, width), BF16))] * Y,
        mflops=400,
    )(at, *routes_two, *logits_two, *cot_two)

    factor = (VMEM, pltpu.HBM((units, rows), F32))
    half_factor = (VMEM, pltpu.HBM((units, rows), BF16))
    preact, up_value, hidden = call(
        forward_body,
        [VMEM, HBM, HBM] + [ANY] * Y,
        [(HBM, pltpu.HBM((units, rows), F32))] * 2 + [(VMEM, sds((units, rows), BF16))],
        [pltpu.VMEM((units, width), BF16)] * 2
        + [pltpu.VMEM((units, rows), F32)] * 2
        + [dma_sems((4,))],
        mflops=704,
    )(slot_x, in_hbm(gate_weight[0]), in_hbm(up_weight[0]), *[in_hbm(v) for v in send_c])

    hidden_parts = spread([hidden] * X, "x")
    partial_out = call(
        down_body,
        [VMEM] * X + [HBM] * X,
        [(HBM, pltpu.HBM((Z * EXPERTS, HALF, 128), BF16))],
        [pltpu.VMEM((units, quarter), BF16)] * X
        + [pltpu.VMEM((Z * EXPERTS, HALF, 128), BF16), dma_sems((X + Z // 2,))],
        mflops=352,
    )(*hidden_parts, *[in_hbm(part) for part in down_parts])

    pieces = spread(send_c, "y")

    back = exchange(partial_out, BACK_AXES)
    *factors, hidden_tang = call(
        tangent_body, [VMEM] * 5, [factor] * 4 + [half_factor], mflops=704
    )(slot_x, in_hbm(preact), in_hbm(up_value), in_hbm(gate_dir), in_hbm(up_dir))
    share = call(
        combine_body, [VMEM] * 3 + [ANY], [(VMEM, pltpu.HBM((Z, 64, tok), BF16))], mflops=100
    )(routes_t, logits_t, back, in_hbm(hidden_tang))
    over_z = exchange(share, "z")
    blocks = spread([over_z] * X, "x")
    mixed = call(
        turn_body, [SMEM] + [VMEM] * X, [(VMEM, sds((tok, width), BF16))], mflops=100
    )(at, *blocks)

    slot_c, resid_gate, resid_up = call(
        residual_body,
        [SMEM] + [VMEM] * (2 + Y + 4),
        [(VMEM, pltpu.HBM((rows, width), BF16)), half_factor, half_factor],
        mflops=904,
    )(at, *[in_hbm(v) for v in (down_mat, down_dir, *pieces, *factors)])
    hold = pltpu.VMEM((1, units, width), F32)
    out = (HBM, pltpu.HBM((1, units, width), F32))
    hvp = call(outer_body, [VMEM] * 5, [out] * 3, [hold] * 3 + [dma_sems((12,))], mflops=1056)(
        in_hbm(resid_gate),
        in_hbm(resid_up),
        in_hbm(hidden_tang),
        slot_x,
        in_hbm(slot_c),
    )
    return (mixed, *hvp)


def solution(mesh):
    grid = Mesh(mesh.devices.reshape(X, Z, Y, 2), ("x", "z", "y", "c"))
    by_expert = P(EXPERT_AXES, None)
    by_both = P(EXPERT_AXES, DP_AXES, None)

    def step(*args):
        return shards(*args)

    step = jax.shard_map(
        step,
        mesh=grid,
        in_specs=(by_expert,) * 4 + (by_both,) * 6,
        out_specs=(by_expert,) + (by_both,) * 3,
        check_vma=False,
    )
    return step
```

```python
import functools

import jax
import jax.numpy as jnp
from jax import lax
from jax.experimental import pallas as pl
from jax.experimental.pallas import tpu as pltpu
from jax.sharding import Mesh, PartitionSpec as P

F32, BF16, I32 = jnp.float32, jnp.bfloat16, jnp.int32
CAP = 48
HALF = CAP // 2
EXPERTS = 8
X, Z, Y = 4, 8, 4
NEAR, FAR = (0, 1, 3), (2,)
VMEM_LIMIT = 16 * 1024 * 1024

DP_AXES = ("x", "z")
EXPERT_AXES = ("y", "c")
BACK_AXES = ("z", "y", "c")

sds = jax.ShapeDtypeStruct
VMEM = pl.BlockSpec(memory_space=pltpu.VMEM)
HBM = pl.BlockSpec(memory_space=pltpu.HBM)
ANY = pl.BlockSpec(memory_space=pl.ANY)


def call(body, ins, outs, scratch=(), mflops=0, **kwargs):
    specs, shapes = [pair[0] for pair in outs], [pair[1] for pair in outs]
    single = len(outs) == 1
    return pl.pallas_call(
        body,
        out_shape=shapes[0] if single else shapes,
        in_specs=ins,
        out_specs=specs[0] if single else specs,
        scratch_shapes=list(scratch),
        cost_estimate=pl.CostEstimate(
            flops=mflops * 1000000, bytes_accessed=4000000, transcendentals=0
        ),
        compiler_params=pltpu.CompilerParams(vmem_limit_bytes=VMEM_LIMIT),
        **kwargs,
    )


def in_hbm(value):
    return pltpu.with_memory_space_constraint(value, pltpu.HBM)


def dma(source, target, sem):
    copy = pltpu.make_async_copy(source, target, sem)
    copy.start()
    return copy


def iota(shape, dim):
    return lax.broadcasted_iota(I32, shape, dim)


def slots_of(routes):
    first, second = routes[0:1, :], routes[1:2, :]
    tok = routes.shape[1]
    experts = iota((EXPERTS, tok), 0)
    is_first, is_second = experts == first, experts == second
    member = jnp.where(is_first | is_second, 1.0, 0.0).astype(BF16)
    before = jnp.where(iota((tok, tok), 0) < iota((tok, tok), 1), 1.0, 0.0).astype(BF16)
    count = jnp.dot(member, before, preferred_element_type=F32)
    pos_first = jnp.sum(jnp.where(is_first, count, 0.0), axis=0, keepdims=True).astype(I32)
    pos_second = jnp.sum(jnp.where(is_second, count, 0.0), axis=0, keepdims=True).astype(I32)
    return first, second, pos_first, pos_second


def gate_probs(logits):
    first = jax.nn.sigmoid(logits[0:1, :] - logits[1:2, :])
    return first, 1.0 - first


def nt_dot(rows, matrix):
    return lax.dot_general(rows, matrix, (((1,), (1,)), ((), ())), preferred_element_type=F32)


def tn_dot(rows, matrix):
    return lax.dot_general(rows, matrix, (((0,), (0,)), ((), ())), preferred_element_type=F32)


def hits(routes, count, row_of):
    first, second, pos_first, pos_second = slots_of(routes)
    rows = iota((count, routes.shape[1]), 0)
    hit = (rows == row_of(first, pos_first)) | (rows == row_of(second, pos_second))
    return jnp.where(hit, 1.0, 0.0).astype(BF16)


def pick_rows(routes, value, count, row_of, weights=None):
    first, second, pos_first, pos_second = slots_of(routes)
    rows = iota((count, value.shape[0]), 0)
    hit_first = rows == row_of(first, pos_first)
    hit_second = rows == row_of(second, pos_second)
    dispatch = jnp.where(hit_first | hit_second, 1.0, 0.0).astype(BF16)
    picked = jnp.dot(dispatch, value, preferred_element_type=F32)
    if weights is not None:
        weight = jnp.where(hit_first, weights[0], 0.0) + jnp.where(hit_second, weights[1], 0.0)
        picked = picked * jnp.sum(weight, axis=1, keepdims=True)
    return picked.astype(BF16)


def send_near_body(routes_hbm, tok_hbm, own_hbm, *refs):
    out_refs, (own_ref, routes_ref, tok_ref, sems) = refs[:-4], refs[-4:]
    get_routes = dma(routes_hbm, routes_ref, sems.at[0])
    get_tok = dma(tok_hbm, tok_ref, sems.at[1])
    y, c = lax.axis_index("y"), lax.axis_index("c")

    def row_of(expert, pos):
        chip = (expert >> 1) ^ y
        block = jnp.where(chip == 3, 2, chip) * 2 + ((expert & 1) ^ c)
        return jnp.where(chip == 2, -1, block * CAP + pos)

    get_routes.wait()
    dispatch = hits(routes_ref[...], len(NEAR) * 2 * CAP, row_of)
    get_tok.wait()
    tokens = tok_ref[...]
    put = None
    for k, ref in enumerate((own_ref, *out_refs)):
        part = dispatch[k * 2 * CAP : (k + 1) * 2 * CAP]
        ref[...] = jnp.dot(part, tokens, preferred_element_type=F32).astype(BF16)
        put = put or dma(own_ref, own_hbm, sems.at[0])
    put.wait()


def send_far_body(*refs):
    routes_refs, tok_refs, out_ref = refs[0:2], refs[2:4], refs[4]
    y, c = lax.axis_index("y"), lax.axis_index("c")

    def row_of(expert, pos):
        wanted = (((expert >> 1) ^ y) == 2) & ((expert & 1) == c)
        return jnp.where(wanted, pos, -1)

    for j in range(2):
        picked = pick_rows(routes_refs[j][...], tok_refs[j][...], CAP, row_of)
        out_ref[j * CAP : (j + 1) * CAP] = picked


def send_cot_body(*refs):
    routes_refs, logits_refs, cot_refs = refs[0:2], refs[2:4], refs[4:6]
    out_refs = refs[6:]
    y, c = lax.axis_index("y"), lax.axis_index("c")

    def row_of(expert, pos):
        return jnp.where((expert & 1) == c, ((expert >> 1) ^ y) * CAP + pos, -1)

    for j in range(2):
        probs = gate_probs(logits_refs[j][...])
        picked = pick_rows(routes_refs[j][...], cot_refs[j][...], Y * CAP, row_of, probs)
        for i, out_ref in enumerate(out_refs):
            out_ref[j * CAP : (j + 1) * CAP] = picked[i * CAP : (i + 1) * CAP]


def split_down_body(down_hbm, own_hbm, *refs):
    out_refs, (own_ref, sems) = refs[:-2], refs[-2:]
    me = lax.axis_index("x")
    width = own_ref.shape[1]
    gets = []
    for i, ref in enumerate((own_ref, *out_refs)):
        start = pl.multiple_of((me ^ i) * width, 128)
        gets.append(dma(down_hbm.at[:, pl.ds(start, width)], ref, sems.at[i]))
    gets[0].wait()
    put = dma(own_ref, own_hbm, sems.at[0])
    for get in gets[1:]:
        get.wait()
    put.wait()


def rows_of(refs):
    return jnp.concatenate([ref[...] for ref in refs], axis=0)


def forward_body(near, *refs):
    count = 2 * len(NEAR) if near else 1
    pieces, (gate_ref, up_ref) = refs[:count], refs[count : count + 2]
    if near:
        parts = [ref[(k % 2) * CAP : (k % 2 + 1) * CAP] for k, ref in enumerate(pieces)]
        pre_hbm, value_hbm, hidden_ref, rows_hbm, pre_ref, value_ref, sems, rows_ref = refs[
            count + 2 :
        ]
        rows = jnp.concatenate(parts, axis=0)
        rows_ref[...] = rows
        puts = [dma(rows_ref, rows_hbm, sems.at[2])]
    else:
        pre_hbm, value_hbm, hidden_ref, pre_ref, value_ref, sems = refs[count + 2 :]
        rows, puts = pieces[0][...], []
    pre = nt_dot(rows, gate_ref[...])
    pre_ref[...] = pre
    puts.append(dma(pre_ref, pre_hbm, sems.at[0]))
    value = nt_dot(rows, up_ref[...])
    value_ref[...] = value
    puts.append(dma(value_ref, value_hbm, sems.at[1]))
    hidden_ref[...] = (pre * jax.nn.sigmoid(pre) * value).astype(BF16)
    for put in puts:
        put.wait()


def down_body(chips, *refs):
    hidden_refs, down_refs = refs[:X], refs[X : 2 * X]
    out_hbm, out_ref, sems = refs[-3:]
    y, c = lax.axis_index("y"), lax.axis_index("c")
    total = None
    for i in range(X):
        part = jnp.dot(hidden_refs[i][...], down_refs[i][...], preferred_element_type=F32)
        total = part if total is None else total + part
    left = iota((HALF, 128), 1) < 64
    puts = []
    for k, chip in enumerate(chips):
        for j in range(2):
            own = 2 * k + j
            for m in range(Z // 2):
                cols = slice(128 * m, 128 * m + 128)
                upper = total[own * CAP : own * CAP + HALF, cols]
                lower = total[own * CAP + HALF : (own + 1) * CAP, cols]
                even = jnp.where(left, upper, pltpu.roll(lower, 64, 1))
                odd = jnp.where(left, pltpu.roll(upper, 64, 1), lower)
                out_ref[own, 2 * m] = even.astype(BF16)
                out_ref[own, 2 * m + 1] = odd.astype(BF16)
            block = 2 * (y ^ chip) + (c ^ j)
            puts.append(dma(out_ref.at[own], out_hbm.at[:, block], sems.at[own]))
    for put in puts:
        put.wait()


def combine_body(routes_ref, logits_ref, back_ref, out_ref):
    first, second, pos_first, pos_second = slots_of(routes_ref[...])
    prob_first, prob_second = gate_probs(logits_ref[...])
    tok = routes_ref.shape[1]
    total = back_ref[0:EXPERTS].astype(F32)
    for z in range(1, Z):
        total = total + back_ref[z * EXPERTS : (z + 1) * EXPERTS].astype(F32)
    held = total.astype(BF16).reshape(EXPERTS * HALF, 128)
    rows = iota((EXPERTS * HALF, tok), 0)

    def pick(expert, pos):
        base = expert * HALF + pos
        in_upper = jnp.where((rows == base) & (pos < HALF), 1.0, 0.0).astype(BF16)
        in_lower = jnp.where((rows == base - HALF) & (pos >= HALF), 1.0, 0.0).astype(BF16)
        return tn_dot(held, in_upper)[0:64] + tn_dot(held, in_lower)[64:128]

    mixed = prob_first * pick(first, pos_first) + prob_second * pick(second, pos_second)
    mixed = mixed.astype(BF16)
    for z in range(Z):
        out_ref[z] = mixed


def turn_body(*refs):
    out_ref = refs[-1]
    me = lax.axis_index("x")
    for i, ref in enumerate(refs[:-1]):
        rows = ref.shape[0] * ref.shape[1]
        block = ref[...].reshape(rows, ref.shape[2])
        for m in range(rows // 128):
            start = pl.multiple_of((me ^ i) * rows + 128 * m, 128)
            out_ref[:, pl.ds(start, 128)] = block[128 * m : 128 * m + 128].T


def tangent_body(*refs):
    piece_refs, pre_refs, value_refs = refs[0:2], refs[2:4], refs[4:6]
    gate_dir_ref, up_dir_ref, *out_refs = refs[6:]
    by_tq_gate_ref, by_q_gate_ref, by_tq_up_ref, by_q_up_ref, hidden_tang_ref = out_refs
    rows = rows_of(piece_refs)
    tang_gate = nt_dot(rows, gate_dir_ref[...])
    tang_up = nt_dot(rows, up_dir_ref[...])
    pre, value = rows_of(pre_refs), rows_of(value_refs)
    sig = jax.nn.sigmoid(pre)
    slope_one = sig * (1.0 + pre * (1.0 - sig))
    slope_two = sig * (1.0 - sig) * (2.0 + pre * (1.0 - 2.0 * sig))
    silu = pre * sig
    silu_tang = slope_one * tang_gate
    by_tq_gate_ref[...] = value * slope_one
    by_q_gate_ref[...] = tang_up * slope_one + value * slope_two * tang_gate
    by_tq_up_ref[...] = silu
    by_q_up_ref[...] = silu_tang
    hidden_tang_ref[...] = (silu_tang * value + silu * tang_up).astype(BF16)


def residual_body(down_ref, down_dir_ref, *refs):
    by_tq_gate_ref, by_q_gate_ref, by_tq_up_ref, by_q_up_ref = refs[Y : Y + 4]
    resid_gate_ref, resid_up_ref = refs[Y + 4 :]
    rows = rows_of(refs[:Y])
    back_grad = nt_dot(rows, down_ref[...])
    back_tang = nt_dot(rows, down_dir_ref[...])
    resid_gate = back_tang * by_tq_gate_ref[...] + back_grad * by_q_gate_ref[...]
    resid_up = back_tang * by_tq_up_ref[...] + back_grad * by_q_up_ref[...]
    resid_gate_ref[...] = resid_gate.astype(BF16)
    resid_up_ref[...] = resid_up.astype(BF16)


def outer_body(gate_units_ref, up_units_ref, down_units_ref, *refs):
    x_refs, c_refs = refs[:2], refs[2 : 2 + Y]
    outs, holds, sems = refs[-7:-4], refs[-4:-1], refs[-1]
    step = x_refs[0].shape[1] // 4
    puts = []
    units = [ref[...].T for ref in (gate_units_ref, up_units_ref, down_units_ref)]
    for g in range(4):
        cols = slice(g * step, (g + 1) * step)
        x_rows = jnp.concatenate([ref[:, cols] for ref in x_refs], axis=0)
        c_rows = jnp.concatenate([ref[:, cols] for ref in c_refs], axis=0)
        for k, rows in enumerate((x_rows, x_rows, c_rows)):
            holds[k][0, :, cols] = jnp.dot(units[k], rows, preferred_element_type=F32)
            where = pl.ds(g * step, step)
            puts.append(
                dma(holds[k].at[:, :, where], outs[k].at[:, :, where], sems.at[3 * g + k])
            )
    for put in puts:
        put.wait()


def spread(pieces, axes):
    arrived = [pieces[0]]
    for i in range(1, len(pieces)):
        pairs = [(d, d ^ i) for d in range(len(pieces))]
        arrived.append(lax.ppermute(pieces[i], axes, pairs))
    return arrived


def exchange(value, axes):
    return lax.all_to_all(value, axes, 0, 0, tiled=True)


def shards(
    tokens,
    cotangent,
    router_logits,
    routes,
    gate_weight,
    up_weight,
    down_weight,
    dir_gate,
    dir_up,
    dir_down,
):
    tok, width = tokens.shape
    rows = EXPERTS * CAP
    units = gate_weight.shape[1]
    quarter = width // X
    routes_t, logits_t = routes.T, router_logits.T
    down_mat = down_weight[0]
    gate_dir, up_dir, down_dir = dir_gate[0], dir_up[0], dir_down[0]
    dma_sems = pltpu.SemaphoreType.DMA

    def pair(value):
        own, other = spread([value] * 2, "c")
        return in_hbm(own), other

    piece = (VMEM, pltpu.HBM((2 * CAP, width), BF16))
    leaves = (VMEM, sds((2 * CAP, width), BF16))
    send_near = call(
        send_near_body,
        [HBM, HBM],
        [(HBM, pltpu.HBM((2 * CAP, width), BF16))]
        + [(VMEM, sds((2 * CAP, width), BF16))] * (len(NEAR) - 1),
        [
            pltpu.VMEM((2 * CAP, width), BF16),
            pltpu.VMEM((2, tok), I32),
            pltpu.VMEM((tok, width), BF16),
            dma_sems((2,)),
        ],
        mflops=200,
    )(in_hbm(routes_t), in_hbm(tokens))
    near_pieces = []
    for i, value in zip(NEAR, send_near):
        if i:
            value = lax.ppermute(value, "y", [(d, d ^ i) for d in range(Y)])
        near_pieces += spread([value] * 2, "c")
    routes_two = pair(routes_t)
    tok_two = pair(tokens)
    send_far = call(send_far_body, [VMEM] * 4, [leaves], mflops=100)(*routes_two, *tok_two)
    far_piece = lax.ppermute(send_far, "y", [(d, d ^ 2) for d in range(Y)])

    send_down = call(
        split_down_body,
        [HBM],
        [(HBM, pltpu.HBM((units, quarter), BF16))]
        + [(VMEM, sds((units, quarter), BF16))] * (X - 1),
        [pltpu.VMEM((units, quarter), BF16), dma_sems((X,))],
        mflops=200,
    )(in_hbm(down_mat))
    down_parts = spread(send_down, "x")
    logits_two = pair(logits_t)
    cot_two = pair(cotangent)
    send_c = call(
        send_cot_body, [VMEM] * 6, [piece] * Y, mflops=400
    )(*routes_two, *logits_two, *cot_two)
    c_pieces = spread(send_c, "y")

    def forward(pieces, near):
        slots = len(pieces) * (CAP if near else 2 * CAP)
        extra = [(HBM, pltpu.HBM((slots, width), BF16))] if near else []
        return call(
            functools.partial(forward_body, near),
            [VMEM] * (len(pieces) + 2),
            [(HBM, pltpu.HBM((slots, units), F32))] * 2
            + [(VMEM, sds((slots, units), BF16))]
            + extra,
            [pltpu.VMEM((slots, units), F32)] * 2
            + [dma_sems((3,))]
            + ([pltpu.VMEM((slots, width), BF16)] if near else []),
            mflops=2 * slots,
        )(*pieces, gate_weight[0], up_weight[0])

    def down(chips, hidden_parts, filled=None):
        extra = [] if filled is None else [in_hbm(filled)]
        return call(
            functools.partial(down_body, chips),
            [VMEM] * (2 * X) + [HBM] * len(extra),
            [(HBM, pltpu.HBM((Z, EXPERTS, HALF, 128), BF16))],
            [
                pltpu.VMEM((2 * len(chips), Z, HALF, 128), BF16),
                dma_sems((2 * len(chips),)),
            ],
            mflops=88 * len(chips),
            input_output_aliases={2 * X: 0} if extra else {},
        )(*hidden_parts, *down_parts, *extra)

    pre_near, value_near, hidden_near, near_rows = forward(near_pieces, True)
    near_parts = spread([hidden_near] * X, "x")
    pre_far, value_far, hidden_far = forward([far_piece], False)
    far_parts = spread([hidden_far] * X, "x")
    filled = down(NEAR, near_parts)
    partial_out = down(FAR, far_parts, filled)

    back = exchange(partial_out.reshape(Z * EXPERTS, HALF, 128), BACK_AXES)
    x_rows = (near_rows, far_piece)
    ordered_c = [c_pieces[i] for i in NEAR + FAR]
    factor = (VMEM, pltpu.HBM((rows, units), F32))
    half_factor = (VMEM, pltpu.HBM((rows, units), BF16))
    *factors, hidden_tang = call(
        tangent_body, [VMEM] * 8, [factor] * 4 + [half_factor], mflops=704
    )(
        *[
            in_hbm(v)
            for v in (*x_rows, pre_near, pre_far, value_near, value_far, gate_dir, up_dir)
        ]
    )
    share = call(
        combine_body, [VMEM] * 3, [(VMEM, pltpu.HBM((Z, 64, tok), BF16))], mflops=100
    )(routes_t, logits_t, back)
    over_z = exchange(share, "z")
    blocks = spread([over_z] * X, "x")
    mixed = call(turn_body, [VMEM] * X, [(VMEM, sds((tok, width), BF16))], mflops=100)(*blocks)

    resid_gate, resid_up = call(
        residual_body, [VMEM] * (2 + Y + 4), [half_factor] * 2, mflops=704
    )(*[in_hbm(v) for v in (down_mat, down_dir, *ordered_c, *factors)])
    hold = pltpu.VMEM((1, units, width), F32)
    out = (HBM, pltpu.HBM((1, units, width), F32))
    hvp = call(
        outer_body, [VMEM] * (5 + Y), [out] * 3, [hold] * 3 + [dma_sems((12,))], mflops=1056
    )(*[in_hbm(v) for v in (resid_gate, resid_up, hidden_tang, *x_rows, *ordered_c)])
    return (mixed, *hvp)


def solution(mesh):
    grid = Mesh(mesh.devices.reshape(X, Z, Y, 2), ("x", "z", "y", "c"))
    by_expert = P(EXPERT_AXES, None)
    by_both = P(EXPERT_AXES, DP_AXES, None)

    def step(*args):
        return shards(*args)

    step = jax.shard_map(
        step,
        mesh=grid,
        in_specs=(by_expert,) * 4 + (by_both,) * 6,
        out_specs=(by_expert,) + (by_both,) * 3,
        check_vma=False,
    )
    return step
```

```python
import functools

import jax
import jax.numpy as jnp
from jax import lax
from jax.experimental import pallas as pl
from jax.experimental.pallas import tpu as pltpu
from jax.sharding import Mesh, PartitionSpec as P

F32, BF16, I32 = jnp.float32, jnp.bfloat16, jnp.int32
CAP = 48
HALF = CAP // 2
EXPERTS = 8
X, Z, Y = 4, 8, 4
NEAR, FAR = (0, 1, 3), (2,)
VMEM_LIMIT = 16 * 1024 * 1024

DP_AXES = ("x", "z")
EXPERT_AXES = ("y", "c")
BACK_AXES = ("z", "y", "c")

sds = jax.ShapeDtypeStruct
VMEM = pl.BlockSpec(memory_space=pltpu.VMEM)
HBM = pl.BlockSpec(memory_space=pltpu.HBM)
ANY = pl.BlockSpec(memory_space=pl.ANY)


def call(body, ins, outs, scratch=(), mflops=0, **kwargs):
    specs, shapes = [pair[0] for pair in outs], [pair[1] for pair in outs]
    single = len(outs) == 1
    return pl.pallas_call(
        body,
        out_shape=shapes[0] if single else shapes,
        in_specs=ins,
        out_specs=specs[0] if single else specs,
        scratch_shapes=list(scratch),
        cost_estimate=pl.CostEstimate(
            flops=mflops * 1000000, bytes_accessed=4000000, transcendentals=0
        ),
        compiler_params=pltpu.CompilerParams(vmem_limit_bytes=VMEM_LIMIT),
        **kwargs,
    )


def in_hbm(value):
    return pltpu.with_memory_space_constraint(value, pltpu.HBM)


def dma(source, target, sem):
    copy = pltpu.make_async_copy(source, target, sem)
    copy.start()
    return copy


def iota(shape, dim):
    return lax.broadcasted_iota(I32, shape, dim)


def slots_of(routes):
    first, second = routes[0:1, :], routes[1:2, :]
    tok = routes.shape[1]
    experts = iota((EXPERTS, tok), 0)
    is_first, is_second = experts == first, experts == second
    member = jnp.where(is_first | is_second, 1.0, 0.0).astype(BF16)
    before = jnp.where(iota((tok, tok), 0) < iota((tok, tok), 1), 1.0, 0.0).astype(BF16)
    count = jnp.dot(member, before, preferred_element_type=F32)
    pos_first = jnp.sum(jnp.where(is_first, count, 0.0), axis=0, keepdims=True).astype(I32)
    pos_second = jnp.sum(jnp.where(is_second, count, 0.0), axis=0, keepdims=True).astype(I32)
    return first, second, pos_first, pos_second


def gate_probs(logits):
    first = jax.nn.sigmoid(logits[0:1, :] - logits[1:2, :])
    return first, 1.0 - first


def nt_dot(rows, matrix):
    return lax.dot_general(rows, matrix, (((1,), (1,)), ((), ())), preferred_element_type=F32)


def tn_dot(rows, matrix):
    return lax.dot_general(rows, matrix, (((0,), (0,)), ((), ())), preferred_element_type=F32)


def hits(routes, count, row_of):
    first, second, pos_first, pos_second = slots_of(routes)
    rows = iota((count, routes.shape[1]), 0)
    hit = (rows == row_of(first, pos_first)) | (rows == row_of(second, pos_second))
    return jnp.where(hit, 1.0, 0.0).astype(BF16)


def pick_rows(routes, value, count, row_of, weights=None):
    first, second, pos_first, pos_second = slots_of(routes)
    rows = iota((count, value.shape[0]), 0)
    hit_first = rows == row_of(first, pos_first)
    hit_second = rows == row_of(second, pos_second)
    dispatch = jnp.where(hit_first | hit_second, 1.0, 0.0).astype(BF16)
    picked = jnp.dot(dispatch, value, preferred_element_type=F32)
    if weights is not None:
        weight = jnp.where(hit_first, weights[0], 0.0) + jnp.where(hit_second, weights[1], 0.0)
        picked = picked * jnp.sum(weight, axis=1, keepdims=True)
    return picked.astype(BF16)


def send_near_body(routes_hbm, tok_hbm, own_hbm, *refs):
    out_refs, (own_ref, routes_ref, tok_ref, sems) = refs[:-4], refs[-4:]
    get_routes = dma(routes_hbm, routes_ref, sems.at[0])
    get_tok = dma(tok_hbm, tok_ref, sems.at[1])
    y, c = lax.axis_index("y"), lax.axis_index("c")

    def row_of(expert, pos):
        chip = (expert >> 1) ^ y
        block = jnp.where(chip == 3, 2, chip) * 2 + ((expert & 1) ^ c)
        return jnp.where(chip == 2, -1, block * CAP + pos)

    get_routes.wait()
    dispatch = hits(routes_ref[...], len(NEAR) * 2 * CAP, row_of)
    get_tok.wait()
    tokens = tok_ref[...]
    put = None
    for k, ref in enumerate((own_ref, *out_refs)):
        part = dispatch[k * 2 * CAP : (k + 1) * 2 * CAP]
        ref[...] = jnp.dot(part, tokens, preferred_element_type=F32).astype(BF16)
        put = put or dma(own_ref, own_hbm, sems.at[0])
    put.wait()


def send_far_body(*refs):
    routes_refs, tok_refs, out_ref = refs[0:2], refs[2:4], refs[4]
    y, c = lax.axis_index("y"), lax.axis_index("c")

    def row_of(expert, pos):
        wanted = (((expert >> 1) ^ y) == 2) & ((expert & 1) == c)
        return jnp.where(wanted, pos, -1)

    for j in range(2):
        picked = pick_rows(routes_refs[j][...], tok_refs[j][...], CAP, row_of)
        out_ref[j * CAP : (j + 1) * CAP] = picked


def send_cot_body(*refs):
    routes_refs, logits_refs, cot_refs = refs[0:2], refs[2:4], refs[4:6]
    out_refs = refs[6:]
    y, c = lax.axis_index("y"), lax.axis_index("c")

    def row_of(expert, pos):
        return jnp.where((expert & 1) == c, ((expert >> 1) ^ y) * CAP + pos, -1)

    for j in range(2):
        probs = gate_probs(logits_refs[j][...])
        picked = pick_rows(routes_refs[j][...], cot_refs[j][...], Y * CAP, row_of, probs)
        for i, out_ref in enumerate(out_refs):
            out_ref[j * CAP : (j + 1) * CAP] = picked[i * CAP : (i + 1) * CAP]


def split_down_body(down_hbm, own_hbm, *refs):
    out_refs, (own_ref, sems) = refs[:-2], refs[-2:]
    me = lax.axis_index("x")
    width = own_ref.shape[1]
    gets = []
    for i, ref in enumerate((own_ref, *out_refs)):
        start = pl.multiple_of((me ^ i) * width, 128)
        gets.append(dma(down_hbm.at[:, pl.ds(start, width)], ref, sems.at[i]))
    gets[0].wait()
    put = dma(own_ref, own_hbm, sems.at[0])
    for get in gets[1:]:
        get.wait()
    put.wait()


def rows_of(refs):
    return jnp.concatenate([ref[...] for ref in refs], axis=0)


def forward_body(near, *refs):
    count = 2 * len(NEAR) if near else 1
    pieces, (gate_ref, up_ref) = refs[:count], refs[count : count + 2]
    if near:
        parts = [ref[(k % 2) * CAP : (k % 2 + 1) * CAP] for k, ref in enumerate(pieces)]
        pre_hbm, value_hbm, hidden_ref, rows_hbm, pre_ref, value_ref, sems, rows_ref = refs[
            count + 2 :
        ]
        rows = jnp.concatenate(parts, axis=0)
        rows_ref[...] = rows
        puts = [dma(rows_ref, rows_hbm, sems.at[2])]
    else:
        pre_hbm, value_hbm, hidden_ref, pre_ref, value_ref, sems = refs[count + 2 :]
        rows, puts = pieces[0][...], []
    pre = nt_dot(rows, gate_ref[...])
    pre_ref[...] = pre
    puts.append(dma(pre_ref, pre_hbm, sems.at[0]))
    value = nt_dot(rows, up_ref[...])
    value_ref[...] = value
    puts.append(dma(value_ref, value_hbm, sems.at[1]))
    hidden_ref[...] = (pre * jax.nn.sigmoid(pre) * value).astype(BF16)
    for put in puts:
        put.wait()


def down_body(chips, *refs):
    hidden_refs, down_refs = refs[:X], refs[X : 2 * X]
    out_hbm, out_ref, sems = refs[-3:]
    y, c = lax.axis_index("y"), lax.axis_index("c")
    total = None
    for i in range(X):
        part = jnp.dot(hidden_refs[i][...], down_refs[i][...], preferred_element_type=F32)
        total = part if total is None else total + part
    left = iota((HALF, 128), 1) < 64
    puts = []
    for k, chip in enumerate(chips):
        for j in range(2):
            own = 2 * k + j
            for m in range(Z // 2):
                cols = slice(128 * m, 128 * m + 128)
                upper = total[own * CAP : own * CAP + HALF, cols]
                lower = total[own * CAP + HALF : (own + 1) * CAP, cols]
                even = jnp.where(left, upper, pltpu.roll(lower, 64, 1))
                odd = jnp.where(left, pltpu.roll(upper, 64, 1), lower)
                out_ref[own, 2 * m] = even.astype(BF16)
                out_ref[own, 2 * m + 1] = odd.astype(BF16)
            block = 2 * (y ^ chip) + (c ^ j)
            puts.append(dma(out_ref.at[own], out_hbm.at[:, block], sems.at[own]))
    for put in puts:
        put.wait()


def combine_body(routes_ref, logits_ref, back_ref, out_ref):
    first, second, pos_first, pos_second = slots_of(routes_ref[...])
    prob_first, prob_second = gate_probs(logits_ref[...])
    tok = routes_ref.shape[1]
    total = back_ref[0:EXPERTS].astype(F32)
    for z in range(1, Z):
        total = total + back_ref[z * EXPERTS : (z + 1) * EXPERTS].astype(F32)
    held = total.astype(BF16).reshape(EXPERTS * HALF, 128)
    rows = iota((EXPERTS * HALF, tok), 0)

    def pick(expert, pos):
        base = expert * HALF + pos
        in_upper = jnp.where((rows == base) & (pos < HALF), 1.0, 0.0).astype(BF16)
        in_lower = jnp.where((rows == base - HALF) & (pos >= HALF), 1.0, 0.0).astype(BF16)
        return tn_dot(held, in_upper)[0:64] + tn_dot(held, in_lower)[64:128]

    mixed = prob_first * pick(first, pos_first) + prob_second * pick(second, pos_second)
    mixed = mixed.astype(BF16)
    for peer in range(X * Z):
        out_ref[peer] = mixed


def turn_body(in_ref, out_ref):
    for m in range(out_ref.shape[1] // 128):
        block = in_ref[2 * m : 2 * m + 2].reshape(128, out_ref.shape[0])
        out_ref[:, 128 * m : 128 * m + 128] = block.T


def tangent_body(*refs):
    piece_refs, pre_refs, value_refs = refs[0:2], refs[2:4], refs[4:6]
    gate_dir_ref, up_dir_ref, *out_refs = refs[6:]
    by_tq_gate_ref, by_q_gate_ref, by_tq_up_ref, by_q_up_ref, hidden_tang_ref = out_refs
    rows = rows_of(piece_refs)
    tang_gate = nt_dot(rows, gate_dir_ref[...])
    tang_up = nt_dot(rows, up_dir_ref[...])
    pre, value = rows_of(pre_refs), rows_of(value_refs)
    sig = jax.nn.sigmoid(pre)
    slope_one = sig * (1.0 + pre * (1.0 - sig))
    slope_two = sig * (1.0 - sig) * (2.0 + pre * (1.0 - 2.0 * sig))
    silu = pre * sig
    silu_tang = slope_one * tang_gate
    by_tq_gate_ref[...] = value * slope_one
    by_q_gate_ref[...] = tang_up * slope_one + value * slope_two * tang_gate
    by_tq_up_ref[...] = silu
    by_q_up_ref[...] = silu_tang
    hidden_tang_ref[...] = (silu_tang * value + silu * tang_up).astype(BF16)


def curvature_body(*refs):
    c_refs, held_hbms, outs = refs[:Y], refs[Y : Y + 9], refs[Y + 9 : Y + 12]
    holds, held_refs, sems = refs[Y + 12 : Y + 15], refs[Y + 15 : Y + 24], refs[Y + 24]
    gets = [dma(a, b, sems.at[12 + i]) for i, (a, b) in enumerate(zip(held_hbms, held_refs))]
    puts = []

    def held(*places):
        for place in places:
            gets[place].wait()
        values = [held_refs[place][...] for place in places]
        return values[0] if len(values) == 1 else values

    def outer(k, units, row_refs):
        units = units.T
        step = row_refs[0].shape[1] // 4
        for g in range(4):
            cols = slice(g * step, (g + 1) * step)
            rows = jnp.concatenate([ref[:, cols] for ref in row_refs], axis=0)
            holds[k][0, :, cols] = jnp.dot(units, rows, preferred_element_type=F32)
            where = pl.ds(g * step, step)
            puts.append(
                dma(holds[k].at[:, :, where], outs[k].at[:, :, where], sems.at[4 * k + g])
            )

    outer(2, held(0), c_refs)
    rows = rows_of(c_refs)
    back_grad = nt_dot(rows, held(1))
    back_tang = nt_dot(rows, held(2))
    by_tq_gate, by_q_gate = held(3, 4)
    resid_gate = back_tang * by_tq_gate + back_grad * by_q_gate
    gets[7].wait()
    gets[8].wait()
    outer(0, resid_gate.astype(BF16), held_refs[7:9])
    by_tq_up, by_q_up = held(5, 6)
    resid_up = back_tang * by_tq_up + back_grad * by_q_up
    outer(1, resid_up.astype(BF16), held_refs[7:9])
    for put in puts:
        put.wait()


def spread(pieces, axes):
    arrived = [pieces[0]]
    for i in range(1, len(pieces)):
        pairs = [(d, d ^ i) for d in range(len(pieces))]
        arrived.append(lax.ppermute(pieces[i], axes, pairs))
    return arrived


def exchange(value, axes):
    return lax.all_to_all(value, axes, 0, 0, tiled=True)


def shards(
    tokens,
    cotangent,
    router_logits,
    routes,
    gate_weight,
    up_weight,
    down_weight,
    dir_gate,
    dir_up,
    dir_down,
):
    tok, width = tokens.shape
    rows = EXPERTS * CAP
    units = gate_weight.shape[1]
    quarter = width // X
    routes_t, logits_t = routes.T, router_logits.T
    down_mat = down_weight[0]
    gate_dir, up_dir, down_dir = dir_gate[0], dir_up[0], dir_down[0]
    dma_sems = pltpu.SemaphoreType.DMA

    def pair(value):
        own, other = spread([value] * 2, "c")
        return in_hbm(own), other

    piece = (VMEM, pltpu.HBM((2 * CAP, width), BF16))
    leaves = (VMEM, sds((2 * CAP, width), BF16))
    send_near = call(
        send_near_body,
        [HBM, HBM],
        [(HBM, pltpu.HBM((2 * CAP, width), BF16))]
        + [(VMEM, sds((2 * CAP, width), BF16))] * (len(NEAR) - 1),
        [
            pltpu.VMEM((2 * CAP, width), BF16),
            pltpu.VMEM((2, tok), I32),
            pltpu.VMEM((tok, width), BF16),
            dma_sems((2,)),
        ],
        mflops=200,
    )(in_hbm(routes_t), in_hbm(tokens))
    near_pieces = []
    for i, value in zip(NEAR, send_near):
        if i:
            value = lax.ppermute(value, "y", [(d, d ^ i) for d in range(Y)])
        near_pieces += spread([value] * 2, "c")
    routes_two = pair(routes_t)
    tok_two = pair(tokens)
    send_far = call(send_far_body, [VMEM] * 4, [leaves], mflops=100)(*routes_two, *tok_two)
    far_piece = lax.ppermute(send_far, "y", [(d, d ^ 2) for d in range(Y)])

    send_down = call(
        split_down_body,
        [HBM],
        [(HBM, pltpu.HBM((units, quarter), BF16))]
        + [(VMEM, sds((units, quarter), BF16))] * (X - 1),
        [pltpu.VMEM((units, quarter), BF16), dma_sems((X,))],
        mflops=200,
    )(in_hbm(down_mat))
    down_parts = spread(send_down, "x")
    logits_two = pair(logits_t)
    cot_two = pair(cotangent)
    send_c = call(
        send_cot_body, [VMEM] * 6, [piece] * Y, mflops=400
    )(*routes_two, *logits_two, *cot_two)
    c_pieces = spread(send_c, "y")

    def forward(pieces, near):
        slots = len(pieces) * (CAP if near else 2 * CAP)
        extra = [(HBM, pltpu.HBM((slots, width), BF16))] if near else []
        return call(
            functools.partial(forward_body, near),
            [VMEM] * (len(pieces) + 2),
            [(HBM, pltpu.HBM((slots, units), F32))] * 2
            + [(VMEM, sds((slots, units), BF16))]
            + extra,
            [pltpu.VMEM((slots, units), F32)] * 2
            + [dma_sems((3,))]
            + ([pltpu.VMEM((slots, width), BF16)] if near else []),
            mflops=2 * slots,
        )(*pieces, gate_weight[0], up_weight[0])

    def down(chips, hidden_parts, filled=None):
        extra = [] if filled is None else [in_hbm(filled)]
        return call(
            functools.partial(down_body, chips),
            [VMEM] * (2 * X) + [HBM] * len(extra),
            [(HBM, pltpu.HBM((Z, EXPERTS, HALF, 128), BF16))],
            [
                pltpu.VMEM((2 * len(chips), Z, HALF, 128), BF16),
                dma_sems((2 * len(chips),)),
            ],
            mflops=88 * len(chips),
            input_output_aliases={2 * X: 0} if extra else {},
        )(*hidden_parts, *down_parts, *extra)

    pre_near, value_near, hidden_near, near_rows = forward(near_pieces, True)
    near_parts = spread([hidden_near] * X, "x")
    pre_far, value_far, hidden_far = forward([far_piece], False)
    far_parts = spread([hidden_far] * X, "x")
    filled = down(NEAR, near_parts)
    partial_out = down(FAR, far_parts, filled)

    back = exchange(partial_out.reshape(Z * EXPERTS, HALF, 128), BACK_AXES)
    x_rows = (near_rows, far_piece)
    ordered_c = [c_pieces[i] for i in NEAR + FAR]
    factor = (VMEM, pltpu.HBM((rows, units), F32))
    half_factor = (VMEM, pltpu.HBM((rows, units), BF16))
    *factors, hidden_tang = call(
        tangent_body, [VMEM] * 8, [factor] * 4 + [half_factor], mflops=704
    )(
        *[
            in_hbm(v)
            for v in (*x_rows, pre_near, pre_far, value_near, value_far, gate_dir, up_dir)
        ]
    )
    share = call(
        combine_body, [VMEM] * 3, [(VMEM, pltpu.HBM((X * Z, 64, tok), BF16))], mflops=100
    )(routes_t, logits_t, back)
    copies = exchange(share, DP_AXES)
    mixed = call(turn_body, [VMEM], [(VMEM, sds((tok, width), BF16))], mflops=100)(copies)

    hold = pltpu.VMEM((1, units, width), F32)
    out = (HBM, pltpu.HBM((1, units, width), F32))
    held = (hidden_tang, down_mat, down_dir, *factors, *x_rows)
    hvp = call(
        curvature_body,
        [VMEM] * Y + [HBM] * len(held),
        [out] * 3,
        [hold] * 3 + [pltpu.VMEM(v.shape, v.dtype) for v in held] + [dma_sems((12 + len(held),))],
        mflops=1760,
    )(*ordered_c, *[in_hbm(v) for v in held])
    return (mixed, *hvp)


def solution(mesh):
    grid = Mesh(mesh.devices.reshape(X, Z, Y, 2), ("x", "z", "y", "c"))
    by_expert = P(EXPERT_AXES, None)
    by_both = P(EXPERT_AXES, DP_AXES, None)

    def step(*args):
        return shards(*args)

    step = jax.shard_map(
        step,
        mesh=grid,
        in_specs=(by_expert,) * 4 + (by_both,) * 6,
        out_specs=(by_expert,) + (by_both,) * 3,
        check_vma=False,
    )
    return step
```

```python
import functools

import jax
import jax.numpy as jnp
from jax import lax
from jax.experimental import pallas as pl
from jax.experimental.pallas import tpu as pltpu
from jax.sharding import Mesh, PartitionSpec as P

F32, BF16, I32 = jnp.float32, jnp.bfloat16, jnp.int32
CAP = 48
HALF = CAP // 2
EXPERTS = 8
X, Z, Y = 4, 8, 4
NEAR, FAR = (0, 1, 3), (2,)
VMEM_LIMIT = 16 * 1024 * 1024

DP_AXES = ("x", "z")
EXPERT_AXES = ("y", "c")
BACK_AXES = ("z", "y", "c")

sds = jax.ShapeDtypeStruct
VMEM = pl.BlockSpec(memory_space=pltpu.VMEM)
HBM = pl.BlockSpec(memory_space=pltpu.HBM)
ANY = pl.BlockSpec(memory_space=pl.ANY)


def call(body, ins, outs, scratch=(), mflops=0, **kwargs):
    specs, shapes = [pair[0] for pair in outs], [pair[1] for pair in outs]
    single = len(outs) == 1
    return pl.pallas_call(
        body,
        out_shape=shapes[0] if single else shapes,
        in_specs=ins,
        out_specs=specs[0] if single else specs,
        scratch_shapes=list(scratch),
        cost_estimate=pl.CostEstimate(
            flops=mflops * 1000000, bytes_accessed=4000000, transcendentals=0
        ),
        compiler_params=pltpu.CompilerParams(vmem_limit_bytes=VMEM_LIMIT),
        **kwargs,
    )


def in_hbm(value):
    return pltpu.with_memory_space_constraint(value, pltpu.HBM)


def dma(source, target, sem):
    copy = pltpu.make_async_copy(source, target, sem)
    copy.start()
    return copy


def iota(shape, dim):
    return lax.broadcasted_iota(I32, shape, dim)


def slots_of(routes):
    first, second = routes[0:1, :], routes[1:2, :]
    tok = routes.shape[1]
    experts = iota((EXPERTS, tok), 0)
    is_first, is_second = experts == first, experts == second
    member = jnp.where(is_first | is_second, 1.0, 0.0).astype(BF16)
    before = jnp.where(iota((tok, tok), 0) < iota((tok, tok), 1), 1.0, 0.0).astype(BF16)
    count = jnp.dot(member, before, preferred_element_type=F32)
    pos_first = jnp.sum(jnp.where(is_first, count, 0.0), axis=0, keepdims=True).astype(I32)
    pos_second = jnp.sum(jnp.where(is_second, count, 0.0), axis=0, keepdims=True).astype(I32)
    return first, second, pos_first, pos_second


def gate_probs(logits):
    first = jax.nn.sigmoid(logits[0:1, :] - logits[1:2, :])
    return first, 1.0 - first


def nt_dot(rows, matrix):
    return lax.dot_general(rows, matrix, (((1,), (1,)), ((), ())), preferred_element_type=F32)


def hits(routes, count, row_of):
    first, second, pos_first, pos_second = slots_of(routes)
    rows = iota((count, routes.shape[1]), 0)
    hit = (rows == row_of(first, pos_first)) | (rows == row_of(second, pos_second))
    return jnp.where(hit, 1.0, 0.0).astype(BF16)


def pick_rows(routes, value, count, row_of, weights=None):
    first, second, pos_first, pos_second = slots_of(routes)
    rows = iota((count, value.shape[0]), 0)
    hit_first = rows == row_of(first, pos_first)
    hit_second = rows == row_of(second, pos_second)
    dispatch = jnp.where(hit_first | hit_second, 1.0, 0.0).astype(BF16)
    picked = jnp.dot(dispatch, value, preferred_element_type=F32)
    if weights is not None:
        weight = jnp.where(hit_first, weights[0], 0.0) + jnp.where(hit_second, weights[1], 0.0)
        picked = picked * jnp.sum(weight, axis=1, keepdims=True)
    return picked.astype(BF16)


def send_near_body(routes_hbm, tok_hbm, own_hbm, *refs):
    out_refs, (own_ref, routes_ref, tok_ref, sems) = refs[:-4], refs[-4:]
    get_routes = dma(routes_hbm, routes_ref, sems.at[0])
    get_tok = dma(tok_hbm, tok_ref, sems.at[1])
    y, c = lax.axis_index("y"), lax.axis_index("c")

    def row_of(expert, pos):
        chip = (expert >> 1) ^ y
        block = jnp.where(chip == 3, 2, chip) * 2 + ((expert & 1) ^ c)
        return jnp.where(chip == 2, -1, block * CAP + pos)

    get_routes.wait()
    dispatch = hits(routes_ref[...], len(NEAR) * 2 * CAP, row_of)
    get_tok.wait()
    tokens = tok_ref[...]
    put = None
    for k, ref in enumerate((own_ref, *out_refs)):
        part = dispatch[k * 2 * CAP : (k + 1) * 2 * CAP]
        ref[...] = jnp.dot(part, tokens, preferred_element_type=F32).astype(BF16)
        put = put or dma(own_ref, own_hbm, sems.at[0])
    put.wait()


def send_far_body(*refs):
    routes_refs, tok_refs, out_ref = refs[0:2], refs[2:4], refs[4]
    y, c = lax.axis_index("y"), lax.axis_index("c")

    def row_of(expert, pos):
        wanted = (((expert >> 1) ^ y) == 2) & ((expert & 1) == c)
        return jnp.where(wanted, pos, -1)

    for j in range(2):
        picked = pick_rows(routes_refs[j][...], tok_refs[j][...], CAP, row_of)
        out_ref[j * CAP : (j + 1) * CAP] = picked


def send_cot_body(j, routes_ref, logits_ref, cot_ref, *refs):
    out_hbms, out_ref, sems = refs[-Y - 2 : -2], refs[-2], refs[-1]
    y, c = lax.axis_index("y"), lax.axis_index("c")

    def row_of(expert, pos):
        return jnp.where((expert & 1) == c, ((expert >> 1) ^ y) * CAP + pos, -1)

    probs = gate_probs(logits_ref[...])
    out_ref[...] = pick_rows(routes_ref[...], cot_ref[...], Y * CAP, row_of, probs)
    puts = [
        dma(out_ref.at[pl.ds(i * CAP, CAP)], out_hbm.at[pl.ds(j * CAP, CAP)], sems.at[i])
        for i, out_hbm in enumerate(out_hbms)
    ]
    for put in puts:
        put.wait()


def split_down_body(down_hbm, own_hbm, *refs):
    out_refs, (own_ref, sems) = refs[:-2], refs[-2:]
    me = lax.axis_index("x")
    width = own_ref.shape[1]
    gets = []
    for i, ref in enumerate((own_ref, *out_refs)):
        start = pl.multiple_of((me ^ i) * width, 128)
        gets.append(dma(down_hbm.at[:, pl.ds(start, width)], ref, sems.at[i]))
    gets[0].wait()
    put = dma(own_ref, own_hbm, sems.at[0])
    for get in gets[1:]:
        get.wait()
    put.wait()


def rows_of(refs):
    return jnp.concatenate([ref[...] for ref in refs], axis=0)


def forward_body(near, *refs):
    count = 2 * len(NEAR) if near else 1
    pieces, (gate_ref, up_ref) = refs[:count], refs[count : count + 2]
    if near:
        parts = [ref[(k % 2) * CAP : (k % 2 + 1) * CAP] for k, ref in enumerate(pieces)]
        pre_hbm, value_hbm, hidden_ref, rows_hbm, pre_ref, value_ref, sems, rows_ref = refs[
            count + 2 :
        ]
        rows = jnp.concatenate(parts, axis=0)
        rows_ref[...] = rows
        puts = [dma(rows_ref, rows_hbm, sems.at[2])]
    else:
        pre_hbm, value_hbm, hidden_ref, pre_ref, value_ref, sems = refs[count + 2 :]
        rows, puts = pieces[0][...], []
    pre = nt_dot(rows, gate_ref[...])
    pre_ref[...] = pre
    puts.append(dma(pre_ref, pre_hbm, sems.at[0]))
    value = nt_dot(rows, up_ref[...])
    value_ref[...] = value
    puts.append(dma(value_ref, value_hbm, sems.at[1]))
    hidden_ref[...] = (pre * jax.nn.sigmoid(pre) * value).astype(BF16)
    for put in puts:
        put.wait()


def down_body(chips, *refs):
    hidden_refs, down_refs = refs[:X], refs[X : 2 * X]
    out_hbm, out_ref, sems = refs[-3:]
    y, c = lax.axis_index("y"), lax.axis_index("c")
    total = None
    for i in range(X):
        part = jnp.dot(hidden_refs[i][...], down_refs[i][...], preferred_element_type=F32)
        total = part if total is None else total + part
    left = iota((HALF, 128), 1) < 64
    puts = []
    for k, chip in enumerate(chips):
        for j in range(2):
            own = 2 * k + j
            for m in range(Z // 2):
                cols = slice(128 * m, 128 * m + 128)
                upper = total[own * CAP : own * CAP + HALF, cols]
                lower = total[own * CAP + HALF : (own + 1) * CAP, cols]
                even = jnp.where(left, upper, pltpu.roll(lower, 64, 1))
                odd = jnp.where(left, pltpu.roll(upper, 64, 1), lower)
                out_ref[own, 2 * m] = even.astype(BF16)
                out_ref[own, 2 * m + 1] = odd.astype(BF16)
            block = 2 * (y ^ chip) + (c ^ j)
            puts.append(dma(out_ref.at[own], out_hbm.at[:, block], sems.at[own]))
    for put in puts:
        put.wait()


def places_body(routes_ref, logits_ref, *out_refs):
    hit_refs, prob_ref = out_refs[:4], out_refs[4]
    first, second, pos_first, pos_second = slots_of(routes_ref[...])
    prob_first, prob_second = gate_probs(logits_ref[...])
    rows = iota((EXPERTS * HALF, routes_ref.shape[1]), 0)
    for k, (expert, pos) in enumerate(((first, pos_first), (second, pos_second))):
        base = expert * HALF + pos
        upper = (rows == base) & (pos < HALF)
        lower = (rows == base - HALF) & (pos >= HALF)
        hit_refs[2 * k][...] = jnp.where(upper, 1.0, 0.0).astype(BF16)
        hit_refs[2 * k + 1][...] = jnp.where(lower, 1.0, 0.0).astype(BF16)
    prob_ref[0:1] = prob_first
    prob_ref[1:2] = prob_second


def combine_body(back_ref, *refs):
    hit_refs, prob_ref, out_hbm, mixed_ref, sem = refs[:4], refs[4], refs[5], refs[6], refs[7]
    total = back_ref[0:EXPERTS].astype(F32)
    for z in range(1, Z):
        total = total + back_ref[z * EXPERTS : (z + 1) * EXPERTS].astype(F32)
    held = total.astype(BF16).reshape(EXPERTS * HALF, 128).T

    def pick(k):
        upper = jnp.dot(held[0:64], hit_refs[2 * k][...], preferred_element_type=F32)
        lower = jnp.dot(held[64:128], hit_refs[2 * k + 1][...], preferred_element_type=F32)
        return upper + lower

    mixed = prob_ref[0:1] * pick(0) + prob_ref[1:2] * pick(1)
    for peer in range(X * Z):
        mixed_ref[peer] = mixed.astype(BF16)
    dma(mixed_ref, out_hbm, sem.at[0]).wait()


def turn_body(in_ref, out_hbm, out_ref, sems):
    puts = []
    for m in range(out_ref.shape[1] // 128):
        block = in_ref[2 * m : 2 * m + 2].reshape(128, out_ref.shape[0])
        out_ref[:, 128 * m : 128 * m + 128] = block.T
        if m % 4 == 3:
            where = pl.ds(512 * (m // 4), 512)
            puts.append(dma(out_ref.at[:, where], out_hbm.at[:, where], sems.at[m // 4]))
    for put in puts:
        put.wait()


def tangent_body(*refs):
    piece_refs, pre_refs, value_refs = refs[0:2], refs[2:4], refs[4:6]
    gate_dir_ref, up_dir_ref, *out_refs = refs[6:]
    by_tq_gate_ref, by_q_gate_ref, by_tq_up_ref, by_q_up_ref, hidden_tang_ref = out_refs
    rows = rows_of(piece_refs)
    tang_gate = nt_dot(rows, gate_dir_ref[...])
    tang_up = nt_dot(rows, up_dir_ref[...])
    pre, value = rows_of(pre_refs), rows_of(value_refs)
    sig = jax.nn.sigmoid(pre)
    slope_one = sig * (1.0 + pre * (1.0 - sig))
    slope_two = sig * (1.0 - sig) * (2.0 + pre * (1.0 - 2.0 * sig))
    silu = pre * sig
    silu_tang = slope_one * tang_gate
    by_tq_gate_ref[...] = value * slope_one
    by_q_gate_ref[...] = tang_up * slope_one + value * slope_two * tang_gate
    by_tq_up_ref[...] = silu
    by_q_up_ref[...] = silu_tang
    hidden_tang_ref[...] = (silu_tang * value + silu * tang_up).astype(BF16)


def curvature_body(*refs):
    c_refs, held_hbms, outs = refs[:Y], refs[Y : Y + 9], refs[Y + 9 : Y + 12]
    holds, held_refs, sems = refs[Y + 12 : Y + 15], refs[Y + 15 : Y + 24], refs[Y + 24]
    gets = [dma(a, b, sems.at[12 + i]) for i, (a, b) in enumerate(zip(held_hbms, held_refs))]
    puts = []

    def held(*places):
        for place in places:
            gets[place].wait()
        values = [held_refs[place][...] for place in places]
        return values[0] if len(values) == 1 else values

    def outer(k, units, row_refs):
        units = units.T
        step = row_refs[0].shape[1] // 4
        for g in range(4):
            cols = slice(g * step, (g + 1) * step)
            rows = jnp.concatenate([ref[:, cols] for ref in row_refs], axis=0)
            holds[k][0, :, cols] = jnp.dot(units, rows, preferred_element_type=F32)
            where = pl.ds(g * step, step)
            puts.append(
                dma(holds[k].at[:, :, where], outs[k].at[:, :, where], sems.at[4 * k + g])
            )

    outer(2, held(0), c_refs)
    rows = rows_of(c_refs)
    back_grad = nt_dot(rows, held(1))
    back_tang = nt_dot(rows, held(2))
    by_tq_gate, by_q_gate = held(3, 4)
    resid_gate = back_tang * by_tq_gate + back_grad * by_q_gate
    gets[7].wait()
    gets[8].wait()
    outer(0, resid_gate.astype(BF16), held_refs[7:9])
    by_tq_up, by_q_up = held(5, 6)
    resid_up = back_tang * by_tq_up + back_grad * by_q_up
    outer(1, resid_up.astype(BF16), held_refs[7:9])
    for put in puts:
        put.wait()


def spread(pieces, axes):
    arrived = [pieces[0]]
    for i in range(1, len(pieces)):
        pairs = [(d, d ^ i) for d in range(len(pieces))]
        arrived.append(lax.ppermute(pieces[i], axes, pairs))
    return arrived


def exchange(value, axes):
    return lax.all_to_all(value, axes, 0, 0, tiled=True)


def shards(
    tokens,
    cotangent,
    router_logits,
    routes,
    gate_weight,
    up_weight,
    down_weight,
    dir_gate,
    dir_up,
    dir_down,
):
    tok, width = tokens.shape
    rows = EXPERTS * CAP
    units = gate_weight.shape[1]
    quarter = width // X
    routes_t, logits_t = routes.T, router_logits.T
    down_mat = down_weight[0]
    gate_dir, up_dir, down_dir = dir_gate[0], dir_up[0], dir_down[0]
    dma_sems = pltpu.SemaphoreType.DMA

    def pair(value):
        own, other = spread([value] * 2, "c")
        return in_hbm(own), other

    piece = (VMEM, pltpu.HBM((2 * CAP, width), BF16))
    leaves = (VMEM, sds((2 * CAP, width), BF16))
    send_near = call(
        send_near_body,
        [HBM, HBM],
        [(HBM, pltpu.HBM((2 * CAP, width), BF16))]
        + [(VMEM, sds((2 * CAP, width), BF16))] * (len(NEAR) - 1),
        [
            pltpu.VMEM((2 * CAP, width), BF16),
            pltpu.VMEM((2, tok), I32),
            pltpu.VMEM((tok, width), BF16),
            dma_sems((2,)),
        ],
        mflops=200,
    )(in_hbm(routes_t), in_hbm(tokens))
    near_pieces = []
    for i, value in zip(NEAR, send_near):
        if i:
            value = lax.ppermute(value, "y", [(d, d ^ i) for d in range(Y)])
        near_pieces += spread([value] * 2, "c")
    routes_two = pair(routes_t)
    tok_two = pair(tokens)
    send_far = call(send_far_body, [VMEM] * 4, [leaves], mflops=100)(*routes_two, *tok_two)
    far_piece = lax.ppermute(send_far, "y", [(d, d ^ 2) for d in range(Y)])

    send_down = call(
        split_down_body,
        [HBM],
        [(HBM, pltpu.HBM((units, quarter), BF16))]
        + [(VMEM, sds((units, quarter), BF16))] * (X - 1),
        [pltpu.VMEM((units, quarter), BF16), dma_sems((X,))],
        mflops=200,
    )(in_hbm(down_mat))
    down_parts = spread(send_down, "x")
    logits_two = pair(logits_t)
    cot_two = pair(cotangent)

    def send_cot(j, filled):
        return call(
            functools.partial(send_cot_body, j),
            [VMEM] * 3 + [HBM] * len(filled),
            [(HBM, pltpu.HBM((2 * CAP, width), BF16))] * Y,
            [pltpu.VMEM((Y * CAP, width), BF16), dma_sems((Y,))],
            mflops=200,
            input_output_aliases={3 + i: i for i in range(len(filled))},
        )(routes_two[j], logits_two[j], cot_two[j], *[in_hbm(value) for value in filled])

    send_c = send_cot(1, send_cot(0, []))
    c_pieces = spread(send_c, "y")

    def forward(pieces, near):
        slots = len(pieces) * (CAP if near else 2 * CAP)
        extra = [(HBM, pltpu.HBM((slots, width), BF16))] if near else []
        return call(
            functools.partial(forward_body, near),
            [VMEM] * (len(pieces) + 2),
            [(HBM, pltpu.HBM((slots, units), F32))] * 2
            + [(VMEM, sds((slots, units), BF16))]
            + extra,
            [pltpu.VMEM((slots, units), F32)] * 2
            + [dma_sems((3,))]
            + ([pltpu.VMEM((slots, width), BF16)] if near else []),
            mflops=2 * slots,
        )(*pieces, gate_weight[0], up_weight[0])

    def down(chips, hidden_parts, filled=None):
        extra = [] if filled is None else [in_hbm(filled)]
        return call(
            functools.partial(down_body, chips),
            [VMEM] * (2 * X) + [HBM] * len(extra),
            [(HBM, pltpu.HBM((Z, EXPERTS, HALF, 128), BF16))],
            [
                pltpu.VMEM((2 * len(chips), Z, HALF, 128), BF16),
                dma_sems((2 * len(chips),)),
            ],
            mflops=88 * len(chips),
            input_output_aliases={2 * X: 0} if extra else {},
        )(*hidden_parts, *down_parts, *extra)

    pre_near, value_near, hidden_near, near_rows = forward(near_pieces, True)
    near_parts = spread([hidden_near] * X, "x")
    pre_far, value_far, hidden_far = forward([far_piece], False)
    far_parts = spread([hidden_far] * X, "x")
    filled = down(NEAR, near_parts)
    partial_out = down(FAR, far_parts, filled)

    back = exchange(partial_out.reshape(Z * EXPERTS, HALF, 128), BACK_AXES)
    x_rows = (near_rows, far_piece)
    ordered_c = [c_pieces[i] for i in NEAR + FAR]
    factor = (VMEM, pltpu.HBM((rows, units), F32))
    half_factor = (VMEM, pltpu.HBM((rows, units), BF16))
    *factors, hidden_tang = call(
        tangent_body, [VMEM] * 8, [factor] * 4 + [half_factor], mflops=704
    )(
        *[
            in_hbm(v)
            for v in (*x_rows, pre_near, pre_far, value_near, value_far, gate_dir, up_dir)
        ]
    )
    half_rows = EXPERTS * HALF
    places = call(
        places_body,
        [VMEM] * 2,
        [(VMEM, sds((half_rows, tok), BF16))] * 4 + [(VMEM, sds((2, tok), F32))],
        mflops=100,
    )(routes_t, logits_t)
    share = call(
        combine_body,
        [VMEM] * 6,
        [(HBM, pltpu.HBM((X * Z, 64, tok), BF16))],
        [pltpu.VMEM((X * Z, 64, tok), BF16), dma_sems((1,))],
        mflops=100,
    )(back, *places)
    copies = exchange(share, DP_AXES)
    mixed = call(
        turn_body,
        [VMEM],
        [(HBM, pltpu.HBM((tok, width), BF16))],
        [pltpu.VMEM((tok, width), BF16), dma_sems((4,))],
        mflops=100,
    )(copies)

    hold = pltpu.VMEM((1, units, width), F32)
    out = (HBM, pltpu.HBM((1, units, width), F32))
    held = (hidden_tang, down_mat, down_dir, *factors, *x_rows)
    hvp = call(
        curvature_body,
        [VMEM] * Y + [HBM] * len(held),
        [out] * 3,
        [hold] * 3 + [pltpu.VMEM(v.shape, v.dtype) for v in held] + [dma_sems((12 + len(held),))],
        mflops=1760,
    )(*ordered_c, *[in_hbm(v) for v in held])
    return (mixed, *hvp)


def solution(mesh):
    grid = Mesh(mesh.devices.reshape(X, Z, Y, 2), ("x", "z", "y", "c"))
    by_expert = P(EXPERT_AXES, None)
    by_both = P(EXPERT_AXES, DP_AXES, None)

    def step(*args):
        return shards(*args)

    step = jax.shard_map(
        step,
        mesh=grid,
        in_specs=(by_expert,) * 4 + (by_both,) * 6,
        out_specs=(by_expert,) + (by_both,) * 3,
        check_vma=False,
    )
    return step
```

```python
import functools

import jax
import jax.numpy as jnp
from jax import lax
from jax.experimental import pallas as pl
from jax.experimental.pallas import tpu as pltpu
from jax.sharding import Mesh, PartitionSpec as P

F32, BF16, I32 = jnp.float32, jnp.bfloat16, jnp.int32
CAP = 48
HALF = CAP // 2
EXPERTS = 8
X, Z, Y = 4, 8, 4
NEAR, FAR = (0, 1, 3), (2,)
VMEM_LIMIT = 16 * 1024 * 1024

DP_AXES = ("x", "z")
EXPERT_AXES = ("y", "c")
BACK_AXES = ("z", "y", "c")

sds = jax.ShapeDtypeStruct
VMEM = pl.BlockSpec(memory_space=pltpu.VMEM)
HBM = pl.BlockSpec(memory_space=pltpu.HBM)
ANY = pl.BlockSpec(memory_space=pl.ANY)


def call(body, ins, outs, scratch=(), mflops=0, **kwargs):
    specs, shapes = [pair[0] for pair in outs], [pair[1] for pair in outs]
    single = len(outs) == 1
    return pl.pallas_call(
        body,
        out_shape=shapes[0] if single else shapes,
        in_specs=ins,
        out_specs=specs[0] if single else specs,
        scratch_shapes=list(scratch),
        cost_estimate=pl.CostEstimate(
            flops=mflops * 1000000, bytes_accessed=4000000, transcendentals=0
        ),
        compiler_params=pltpu.CompilerParams(vmem_limit_bytes=VMEM_LIMIT),
        **kwargs,
    )


def in_hbm(value):
    return pltpu.with_memory_space_constraint(value, pltpu.HBM)


def dma(source, target, sem):
    copy = pltpu.make_async_copy(source, target, sem)
    copy.start()
    return copy


def iota(shape, dim):
    return lax.broadcasted_iota(I32, shape, dim)


def slots_of(routes):
    first, second = routes[0:1, :], routes[1:2, :]
    tok = routes.shape[1]
    experts = iota((EXPERTS, tok), 0)
    is_first, is_second = experts == first, experts == second
    member = jnp.where(is_first | is_second, 1.0, 0.0).astype(BF16)
    before = jnp.where(iota((tok, tok), 0) < iota((tok, tok), 1), 1.0, 0.0).astype(BF16)
    count = jnp.dot(member, before, preferred_element_type=F32)
    pos_first = jnp.sum(jnp.where(is_first, count, 0.0), axis=0, keepdims=True).astype(I32)
    pos_second = jnp.sum(jnp.where(is_second, count, 0.0), axis=0, keepdims=True).astype(I32)
    return first, second, pos_first, pos_second


def sigmoid(value):
    small = jnp.exp(-jnp.abs(value))
    return jnp.where(value >= 0.0, 1.0, small) / (1.0 + small)


def gate_probs(logits):
    first = sigmoid(logits[0:1, :] - logits[1:2, :])
    return first, 1.0 - first


def nt_dot(rows, matrix):
    return lax.dot_general(rows, matrix, (((1,), (1,)), ((), ())), preferred_element_type=F32)


def hits(routes, count, row_of):
    first, second, pos_first, pos_second = slots_of(routes)
    rows = iota((count, routes.shape[1]), 0)
    hit = (rows == row_of(first, pos_first)) | (rows == row_of(second, pos_second))
    return jnp.where(hit, 1.0, 0.0).astype(BF16)


def pick_rows(routes, value, count, row_of, weights=None):
    first, second, pos_first, pos_second = slots_of(routes)
    rows = iota((count, value.shape[0]), 0)
    hit_first = rows == row_of(first, pos_first)
    hit_second = rows == row_of(second, pos_second)
    dispatch = jnp.where(hit_first | hit_second, 1.0, 0.0).astype(BF16)
    picked = jnp.dot(dispatch, value, preferred_element_type=F32)
    if weights is not None:
        weight = jnp.where(hit_first, weights[0], 0.0) + jnp.where(hit_second, weights[1], 0.0)
        picked = picked * jnp.sum(weight, axis=1, keepdims=True)
    return picked.astype(BF16)


def send_near_body(routes_hbm, tok_hbm, own_hbm, *refs):
    out_refs, (own_ref, routes_ref, tok_ref, sems) = refs[:-4], refs[-4:]
    get_routes = dma(routes_hbm, routes_ref, sems.at[0])
    get_tok = dma(tok_hbm, tok_ref, sems.at[1])
    y, c = lax.axis_index("y"), lax.axis_index("c")

    def row_of(expert, pos):
        chip = (expert >> 1) ^ y
        block = jnp.where(chip == 3, 2, chip) * 2 + ((expert & 1) ^ c)
        return jnp.where(chip == 2, -1, block * CAP + pos)

    get_routes.wait()
    dispatch = hits(routes_ref[...], len(NEAR) * 2 * CAP, row_of)
    get_tok.wait()
    tokens = tok_ref[...]
    put = None
    for k, ref in enumerate((own_ref, *out_refs)):
        part = dispatch[k * 2 * CAP : (k + 1) * 2 * CAP]
        ref[...] = jnp.dot(part, tokens, preferred_element_type=F32).astype(BF16)
        put = put or dma(own_ref, own_hbm, sems.at[0])
    put.wait()


def send_far_body(*refs):
    routes_refs, tok_refs, out_ref = refs[0:2], refs[2:4], refs[4]
    y, c = lax.axis_index("y"), lax.axis_index("c")

    def row_of(expert, pos):
        wanted = (((expert >> 1) ^ y) == 2) & ((expert & 1) == c)
        return jnp.where(wanted, pos, -1)

    for j in range(2):
        picked = pick_rows(routes_refs[j][...], tok_refs[j][...], CAP, row_of)
        out_ref[j * CAP : (j + 1) * CAP] = picked


def send_cot_body(j, routes_ref, logits_ref, cot_ref, *refs):
    out_hbms, out_ref, sems = refs[-Y - 2 : -2], refs[-2], refs[-1]
    y, c = lax.axis_index("y"), lax.axis_index("c")

    def row_of(expert, pos):
        return jnp.where((expert & 1) == c, ((expert >> 1) ^ y) * CAP + pos, -1)

    probs = gate_probs(logits_ref[...])
    out_ref[...] = pick_rows(routes_ref[...], cot_ref[...], Y * CAP, row_of, probs)
    puts = [
        dma(out_ref.at[pl.ds(i * CAP, CAP)], out_hbm.at[pl.ds(j * CAP, CAP)], sems.at[i])
        for i, out_hbm in enumerate(out_hbms)
    ]
    for put in puts:
        put.wait()


def split_down_body(down_hbm, own_hbm, *refs):
    out_refs, (own_ref, sems) = refs[:-2], refs[-2:]
    me = lax.axis_index("x")
    width = own_ref.shape[1]
    gets = []
    for i, ref in enumerate((own_ref, *out_refs)):
        start = pl.multiple_of((me ^ i) * width, 128)
        gets.append(dma(down_hbm.at[:, pl.ds(start, width)], ref, sems.at[i]))
    gets[0].wait()
    put = dma(own_ref, own_hbm, sems.at[0])
    for get in gets[1:]:
        get.wait()
    put.wait()


def rows_of(refs):
    return jnp.concatenate([ref[...] for ref in refs], axis=0)


def forward_body(near, *refs):
    count = 2 * len(NEAR) if near else 1
    pieces, (gate_ref, up_ref) = refs[:count], refs[count : count + 2]
    if near:
        parts = [ref[(k % 2) * CAP : (k % 2 + 1) * CAP] for k, ref in enumerate(pieces)]
        pre_hbm, value_hbm, hidden_ref, rows_hbm, pre_ref, value_ref, sems, rows_ref = refs[
            count + 2 :
        ]
        rows = jnp.concatenate(parts, axis=0)
        rows_ref[...] = rows
        puts = [dma(rows_ref, rows_hbm, sems.at[2])]
    else:
        pre_hbm, value_hbm, hidden_ref, pre_ref, value_ref, sems = refs[count + 2 :]
        rows, puts = pieces[0][...], []
    pre = nt_dot(rows, gate_ref[...])
    pre_ref[...] = pre
    puts.append(dma(pre_ref, pre_hbm, sems.at[0]))
    value = nt_dot(rows, up_ref[...])
    value_ref[...] = value
    puts.append(dma(value_ref, value_hbm, sems.at[1]))
    hidden_ref[...] = (pre * sigmoid(pre) * value).astype(BF16)
    for put in puts:
        put.wait()


def down_body(chips, *refs):
    hidden_refs, down_refs = refs[:X], refs[X : 2 * X]
    out_hbm, out_ref, sems = refs[-3:]
    y, c = lax.axis_index("y"), lax.axis_index("c")
    total = None
    for i in range(X):
        part = jnp.dot(hidden_refs[i][...], down_refs[i][...], preferred_element_type=F32)
        total = part if total is None else total + part
    left = iota((HALF, 128), 1) < 64
    puts = []
    for k, chip in enumerate(chips):
        for j in range(2):
            own = 2 * k + j
            for m in range(Z // 2):
                cols = slice(128 * m, 128 * m + 128)
                upper = total[own * CAP : own * CAP + HALF, cols]
                lower = total[own * CAP + HALF : (own + 1) * CAP, cols]
                even = jnp.where(left, upper, pltpu.roll(lower, 64, 1))
                odd = jnp.where(left, pltpu.roll(upper, 64, 1), lower)
                out_ref[own, 2 * m] = even.astype(BF16)
                out_ref[own, 2 * m + 1] = odd.astype(BF16)
            block = 2 * (y ^ chip) + (c ^ j)
            puts.append(dma(out_ref.at[own], out_hbm.at[:, block], sems.at[own]))
    for put in puts:
        put.wait()


def places_body(routes_ref, logits_ref, *out_refs):
    hit_refs, prob_ref = out_refs[:4], out_refs[4]
    first, second, pos_first, pos_second = slots_of(routes_ref[...])
    prob_first, prob_second = gate_probs(logits_ref[...])
    rows = iota((EXPERTS * HALF, routes_ref.shape[1]), 0)
    for k, (expert, pos) in enumerate(((first, pos_first), (second, pos_second))):
        base = expert * HALF + pos
        upper = (rows == base) & (pos < HALF)
        lower = (rows == base - HALF) & (pos >= HALF)
        hit_refs[2 * k][...] = jnp.where(upper, 1.0, 0.0).astype(BF16)
        hit_refs[2 * k + 1][...] = jnp.where(lower, 1.0, 0.0).astype(BF16)
    prob_ref[0:1] = prob_first
    prob_ref[1:2] = prob_second


def combine_body(back_ref, *refs):
    hit_refs, prob_ref, out_hbm, mixed_ref, sem = refs[:4], refs[4], refs[5], refs[6], refs[7]
    total = back_ref[0:EXPERTS].astype(F32)
    for z in range(1, Z):
        total = total + back_ref[z * EXPERTS : (z + 1) * EXPERTS].astype(F32)
    held = total.astype(BF16).reshape(EXPERTS * HALF, 128).T

    def pick(k):
        upper = jnp.dot(held[0:64], hit_refs[2 * k][...], preferred_element_type=F32)
        lower = jnp.dot(held[64:128], hit_refs[2 * k + 1][...], preferred_element_type=F32)
        return upper + lower

    mixed = prob_ref[0:1] * pick(0) + prob_ref[1:2] * pick(1)
    for peer in range(X * Z):
        mixed_ref[peer] = mixed.astype(BF16)
    dma(mixed_ref, out_hbm, sem.at[0]).wait()


def turn_body(in_ref, out_hbm, out_ref, sems):
    puts = []
    for m in range(out_ref.shape[1] // 128):
        block = in_ref[2 * m : 2 * m + 2].reshape(128, out_ref.shape[0])
        out_ref[:, 128 * m : 128 * m + 128] = block.T
        if m % 4 == 3:
            where = pl.ds(512 * (m // 4), 512)
            puts.append(dma(out_ref.at[:, where], out_hbm.at[:, where], sems.at[m // 4]))
    for put in puts:
        put.wait()


def tangent_body(*refs):
    piece_refs, pre_refs, value_refs = refs[0:2], refs[2:4], refs[4:6]
    gate_dir_ref, up_dir_ref, *out_refs = refs[6:]
    by_tq_gate_ref, by_q_gate_ref, by_tq_up_ref, by_q_up_ref, hidden_tang_ref = out_refs
    rows = rows_of(piece_refs)
    tang_gate = nt_dot(rows, gate_dir_ref[...])
    tang_up = nt_dot(rows, up_dir_ref[...])
    pre, value = rows_of(pre_refs), rows_of(value_refs)
    sig = sigmoid(pre)
    slope_one = sig * (1.0 + pre * (1.0 - sig))
    slope_two = sig * (1.0 - sig) * (2.0 + pre * (1.0 - 2.0 * sig))
    silu = pre * sig
    silu_tang = slope_one * tang_gate
    by_tq_gate_ref[...] = value * slope_one
    by_q_gate_ref[...] = tang_up * slope_one + value * slope_two * tang_gate
    by_tq_up_ref[...] = silu
    by_q_up_ref[...] = silu_tang
    hidden_tang_ref[...] = (silu_tang * value + silu * tang_up).astype(BF16)


def curvature_body(*refs):
    c_refs, held_hbms, outs = refs[:Y], refs[Y : Y + 9], refs[Y + 9 : Y + 12]
    holds, held_refs, sems = refs[Y + 12 : Y + 15], refs[Y + 15 : Y + 24], refs[Y + 24]
    gets = [dma(a, b, sems.at[12 + i]) for i, (a, b) in enumerate(zip(held_hbms, held_refs))]
    puts = []

    def held(*places):
        for place in places:
            gets[place].wait()
        values = [held_refs[place][...] for place in places]
        return values[0] if len(values) == 1 else values

    def outer(k, units, row_refs):
        units = units.T
        step = row_refs[0].shape[1] // 4
        for g in range(4):
            cols = slice(g * step, (g + 1) * step)
            rows = jnp.concatenate([ref[:, cols] for ref in row_refs], axis=0)
            holds[k][0, :, cols] = jnp.dot(units, rows, preferred_element_type=F32)
            where = pl.ds(g * step, step)
            puts.append(
                dma(holds[k].at[:, :, where], outs[k].at[:, :, where], sems.at[4 * k + g])
            )

    outer(2, held(0), c_refs)
    rows = rows_of(c_refs)
    back_grad = nt_dot(rows, held(1))
    back_tang = nt_dot(rows, held(2))
    by_tq_gate, by_q_gate = held(3, 4)
    resid_gate = back_tang * by_tq_gate + back_grad * by_q_gate
    gets[7].wait()
    gets[8].wait()
    outer(0, resid_gate.astype(BF16), held_refs[7:9])
    by_tq_up, by_q_up = held(5, 6)
    resid_up = back_tang * by_tq_up + back_grad * by_q_up
    outer(1, resid_up.astype(BF16), held_refs[7:9])
    for put in puts:
        put.wait()


def spread(pieces, axes):
    arrived = [pieces[0]]
    for i in range(1, len(pieces)):
        pairs = [(d, d ^ i) for d in range(len(pieces))]
        arrived.append(lax.ppermute(pieces[i], axes, pairs))
    return arrived


def exchange(value, axes):
    return lax.all_to_all(value, axes, 0, 0, tiled=True)


def shards(
    tokens,
    cotangent,
    router_logits,
    routes,
    gate_weight,
    up_weight,
    down_weight,
    dir_gate,
    dir_up,
    dir_down,
):
    tok, width = tokens.shape
    rows = EXPERTS * CAP
    units = gate_weight.shape[1]
    quarter = width // X
    routes_t, logits_t = routes.T, router_logits.T
    down_mat = down_weight[0]
    gate_dir, up_dir, down_dir = dir_gate[0], dir_up[0], dir_down[0]
    dma_sems = pltpu.SemaphoreType.DMA

    def pair(value):
        own, other = spread([value] * 2, "c")
        return in_hbm(own), other

    piece = (VMEM, pltpu.HBM((2 * CAP, width), BF16))
    leaves = (VMEM, sds((2 * CAP, width), BF16))
    send_near = call(
        send_near_body,
        [HBM, HBM],
        [(HBM, pltpu.HBM((2 * CAP, width), BF16))]
        + [(VMEM, sds((2 * CAP, width), BF16))] * (len(NEAR) - 1),
        [
            pltpu.VMEM((2 * CAP, width), BF16),
            pltpu.VMEM((2, tok), I32),
            pltpu.VMEM((tok, width), BF16),
            dma_sems((2,)),
        ],
        mflops=200,
    )(in_hbm(routes_t), in_hbm(tokens))
    near_pieces = []
    for i, value in zip(NEAR, send_near):
        if i:
            value = lax.ppermute(value, "y", [(d, d ^ i) for d in range(Y)])
        near_pieces += spread([value] * 2, "c")
    routes_two = pair(routes_t)
    tok_two = pair(tokens)
    send_far = call(send_far_body, [VMEM] * 4, [leaves], mflops=100)(*routes_two, *tok_two)
    far_piece = lax.ppermute(send_far, "y", [(d, d ^ 2) for d in range(Y)])

    send_down = call(
        split_down_body,
        [HBM],
        [(HBM, pltpu.HBM((units, quarter), BF16))]
        + [(VMEM, sds((units, quarter), BF16))] * (X - 1),
        [pltpu.VMEM((units, quarter), BF16), dma_sems((X,))],
        mflops=200,
    )(in_hbm(down_mat))
    down_parts = spread(send_down, "x")
    logits_two = pair(logits_t)
    cot_two = pair(cotangent)

    def send_cot(j, filled):
        return call(
            functools.partial(send_cot_body, j),
            [VMEM] * 3 + [HBM] * len(filled),
            [(HBM, pltpu.HBM((2 * CAP, width), BF16))] * Y,
            [pltpu.VMEM((Y * CAP, width), BF16), dma_sems((Y,))],
            mflops=200,
            input_output_aliases={3 + i: i for i in range(len(filled))},
        )(routes_two[j], logits_two[j], cot_two[j], *[in_hbm(value) for value in filled])

    send_c = send_cot(1, send_cot(0, []))
    c_pieces = spread(send_c, "y")

    def forward(pieces, near):
        slots = len(pieces) * (CAP if near else 2 * CAP)
        extra = [(HBM, pltpu.HBM((slots, width), BF16))] if near else []
        return call(
            functools.partial(forward_body, near),
            [VMEM] * (len(pieces) + 2),
            [(HBM, pltpu.HBM((slots, units), F32))] * 2
            + [(VMEM, sds((slots, units), BF16))]
            + extra,
            [pltpu.VMEM((slots, units), F32)] * 2
            + [dma_sems((3,))]
            + ([pltpu.VMEM((slots, width), BF16)] if near else []),
            mflops=2 * slots,
        )(*pieces, gate_weight[0], up_weight[0])

    def down(chips, hidden_parts, filled=None):
        extra = [] if filled is None else [in_hbm(filled)]
        return call(
            functools.partial(down_body, chips),
            [VMEM] * (2 * X) + [HBM] * len(extra),
            [(HBM, pltpu.HBM((Z, EXPERTS, HALF, 128), BF16))],
            [
                pltpu.VMEM((2 * len(chips), Z, HALF, 128), BF16),
                dma_sems((2 * len(chips),)),
            ],
            mflops=88 * len(chips),
            input_output_aliases={2 * X: 0} if extra else {},
        )(*hidden_parts, *down_parts, *extra)

    pre_near, value_near, hidden_near, near_rows = forward(near_pieces, True)
    near_parts = spread([hidden_near] * X, "x")
    pre_far, value_far, hidden_far = forward([far_piece], False)
    far_parts = spread([hidden_far] * X, "x")
    filled = down(NEAR, near_parts)
    partial_out = down(FAR, far_parts, filled)

    back = exchange(partial_out.reshape(Z * EXPERTS, HALF, 128), BACK_AXES)
    x_rows = (near_rows, far_piece)
    ordered_c = [c_pieces[i] for i in NEAR + FAR]
    factor = (VMEM, pltpu.HBM((rows, units), F32))
    half_factor = (VMEM, pltpu.HBM((rows, units), BF16))
    *factors, hidden_tang = call(
        tangent_body, [VMEM] * 8, [factor] * 4 + [half_factor], mflops=704
    )(
        *[
            in_hbm(v)
            for v in (*x_rows, pre_near, pre_far, value_near, value_far, gate_dir, up_dir)
        ]
    )
    half_rows = EXPERTS * HALF
    places = call(
        places_body,
        [VMEM] * 2,
        [(VMEM, sds((half_rows, tok), BF16))] * 4 + [(VMEM, sds((2, tok), F32))],
        mflops=100,
    )(routes_t, logits_t)
    share = call(
        combine_body,
        [VMEM] * 6,
        [(HBM, pltpu.HBM((X * Z, 64, tok), BF16))],
        [pltpu.VMEM((X * Z, 64, tok), BF16), dma_sems((1,))],
        mflops=100,
    )(back, *places)
    copies = exchange(share, DP_AXES)
    mixed = call(
        turn_body,
        [VMEM],
        [(HBM, pltpu.HBM((tok, width), BF16))],
        [pltpu.VMEM((tok, width), BF16), dma_sems((4,))],
        mflops=100,
    )(copies)

    hold = pltpu.VMEM((1, units, width), F32)
    out = (HBM, pltpu.HBM((1, units, width), F32))
    held = (hidden_tang, down_mat, down_dir, *factors, *x_rows)
    hvp = call(
        curvature_body,
        [VMEM] * Y + [HBM] * len(held),
        [out] * 3,
        [hold] * 3 + [pltpu.VMEM(v.shape, v.dtype) for v in held] + [dma_sems((12 + len(held),))],
        mflops=1760,
    )(*ordered_c, *[in_hbm(v) for v in held])
    return (mixed, *hvp)


def solution(mesh):
    grid = Mesh(mesh.devices.reshape(X, Z, Y, 2), ("x", "z", "y", "c"))
    by_expert = P(EXPERT_AXES, None)
    by_both = P(EXPERT_AXES, DP_AXES, None)

    def step(*args):
        return shards(*args)

    step = jax.shard_map(
        step,
        mesh=grid,
        in_specs=(by_expert,) * 4 + (by_both,) * 6,
        out_specs=(by_expert,) + (by_both,) * 3,
        check_vma=False,
    )
    return step
```
